32 devices in a mesh: gx: 4 (over y, x), gy: 2 (over core), ha: 4 (over z).
Axes of the slice: x: 2, y: 2, z: 4, core: 2. Of those that a mesh axis runs over, the one named last changes fastest.
Arguments:
- level_set: float32 [32, 32, 40, 128], P('gx', 'gy', 'ha'), may hold values from -4 to 4
- wind_field: float32 [2, 32, 32], P(None, 'gx', 'gy'), may hold values from -3 to 3
Outputs:
- increment: float32 [32, 32, 40, 128], P('gx', 'gy', 'ha')
The draws below stay inside these ranges and needn't reach their ends.
All inputs are finite; a program needn't handle non-finite values.
Results may differ from the reference program's by a relative error of at most 0.000073.
Values sent between devices are 32-bit elements; how exact they have to be, the bound alone decides.
A program may use at most 128 MiB of HBM per device.

```python
import math
import jax
import jax.numpy as jnp
from jax import lax

NV = 128
NX = 32
NY = 32
NH = 40


CELL_SIZE = 0.05


def draw_level_set(key, part):
    rough_key = jax.random.fold_in(key, 11)
    center_key = jax.random.fold_in(key, 12)
    shape = (NX, NY, NH, NV)
    centers = jax.random.uniform(center_key, (2,), jnp.float32, 0.3, 0.7)
    pos_x = (jnp.arange(NX, dtype=jnp.float32) + 0.5) / NX
    pos_y = (jnp.arange(NY, dtype=jnp.float32) + 0.5) / NY
    span_x = (pos_x - centers[0]) * NX * CELL_SIZE
    span_y = (pos_y - centers[1]) * NY * CELL_SIZE
    smooth = jnp.sqrt(span_x[:, None] ** 2 + span_y[None, :] ** 2 + 0.01) - 0.25 * NX * CELL_SIZE
    smooth = smooth[:, :, None, None]
    rough = 0.5 * jax.random.normal(rough_key, shape, jnp.float32)
    surface = rough + smooth
    return jnp.clip(surface, -4.0, 4.0)


def draw_wind_field(key, part):
    raw_key = jax.random.fold_in(key, 21)
    shape = (2, NX, NY)
    ramp = 0.1 + 2.9 * (jnp.arange(NX, dtype=jnp.float32) + 0.5) / NX
    raw = jax.random.uniform(raw_key, shape, jnp.float32, -1.0, 1.0)
    return raw * ramp[None, :, None]


def setup_inputs(seed: int = 0) -> dict:
    streams_of = jax.random.split(jax.random.key(seed), 3)
    return {
        "level_set": draw_level_set(jax.random.fold_in(streams_of[2], 71), 0),
        "wind_field": draw_wind_field(jax.random.fold_in(streams_of[2], 71), 0),
    }


CELL_SIZE = 0.05
SPEED_LOW = 0.1
SPEED_SPAN = 0.4
TURN_MAX = 1.0
ACCEL_MAX = 0.05
CFL_NUMBER = 0.5
WENO_EPS = 1e-6


def ghost_rows(values, along, at_low):
    length = values.shape[along]
    if at_low:
        edge_row = lax.slice_in_dim(values, 0, 1, axis=along)
        next_row = lax.slice_in_dim(values, 1, 2, axis=along)
        reaches = (3.0, 2.0, 1.0)
    else:
        edge_row = lax.slice_in_dim(values, length - 1, length, axis=along)
        next_row = lax.slice_in_dim(values, length - 2, length - 1, axis=along)
        reaches = (1.0, 2.0, 3.0)
    slope_edge = edge_row - next_row
    return jnp.concatenate([edge_row + distance * slope_edge for distance in reaches], axis=along)


def extend(values, along):
    return jnp.concatenate([ghost_rows(values, along, True), values, ghost_rows(values, along, False)], axis=along)


def speed_shifts(values):
    length = values.shape[3]
    below_rows = ghost_rows(values, 3, True)
    above_rows = ghost_rows(values, 3, False)
    shifted = []
    for displace in range(-3, 4):
        pieces = []
        if displace < 0:
            pieces.append(lax.slice_in_dim(below_rows, 3 + displace, 3, axis=3))
        pieces.append(lax.slice_in_dim(values, max(displace, 0), length + min(displace, 0), axis=3))
        if displace > 0:
            pieces.append(lax.slice_in_dim(above_rows, 0, displace, axis=3))
        shifted.append(jnp.concatenate(pieces, axis=3) if len(pieces) > 1 else pieces[0])
    return shifted


def weno_side(left_far, left_near, middle, right_near, right_far):
    guess_one = left_far * (1.0 / 3.0) - left_near * (7.0 / 6.0) + middle * (11.0 / 6.0)
    guess_two = -left_near * (1.0 / 6.0) + middle * (5.0 / 6.0) + right_near * (1.0 / 3.0)
    guess_three = middle * (1.0 / 3.0) + right_near * (5.0 / 6.0) - right_far * (1.0 / 6.0)
    smooth_one = (13.0 / 12.0) * jnp.square(left_far - 2.0 * left_near + middle) + 0.25 * jnp.square(left_far - 4.0 * left_near + 3.0 * middle)
    smooth_two = (13.0 / 12.0) * jnp.square(left_near - 2.0 * middle + right_near) + 0.25 * jnp.square(left_near - right_near)
    smooth_three = (13.0 / 12.0) * jnp.square(middle - 2.0 * right_near + right_far) + 0.25 * jnp.square(3.0 * middle - 4.0 * right_near + right_far)
    weight_one = 0.1 / jnp.square(smooth_one + WENO_EPS)
    weight_two = 0.6 / jnp.square(smooth_two + WENO_EPS)
    weight_three = 0.3 / jnp.square(smooth_three + WENO_EPS)
    return (weight_one * guess_one + weight_two * guess_two + weight_three * guess_three) / (weight_one + weight_two + weight_three)


def weno_pair(shifted, spacing):
    slopes = [(shifted[position + 1] - shifted[position]) / spacing for position in range(6)]
    left_slope = weno_side(slopes[0], slopes[1], slopes[2], slopes[3], slopes[4])
    right_slope = weno_side(slopes[5], slopes[4], slopes[3], slopes[2], slopes[1])
    return left_slope, right_slope


def cell_rates(cos_head, sin_head, speeds, wind_x, wind_y, d_theta, d_speed):
    along_x = speeds[None, None, None, :] * cos_head[None, None, :, None] + wind_x[:, :, None, None]
    along_y = speeds[None, None, None, :] * sin_head[None, None, :, None] + wind_y[:, :, None, None]
    return jnp.abs(along_x) / CELL_SIZE + jnp.abs(along_y) / CELL_SIZE + TURN_MAX / d_theta + ACCEL_MAX / d_speed


def hamilton(x_pair, y_pair, head_pair, speed_pair, cos_head, sin_head, speeds, wind_x, wind_y):
    flow_x = speeds[None, None, None, :] * cos_head[None, None, :, None] + wind_x[:, :, None, None]
    flow_y = speeds[None, None, None, :] * sin_head[None, None, :, None] + wind_y[:, :, None, None]
    mean_x = 0.5 * (x_pair[0] + x_pair[1])
    mean_y = 0.5 * (y_pair[0] + y_pair[1])
    mean_head = 0.5 * (head_pair[0] + head_pair[1])
    mean_speed = 0.5 * (speed_pair[0] + speed_pair[1])
    value = -(flow_x * mean_x + flow_y * mean_y + TURN_MAX * jnp.abs(mean_head) + ACCEL_MAX * jnp.abs(mean_speed))
    damping = 0.5 * (jnp.abs(flow_x) * (x_pair[1] - x_pair[0]) + jnp.abs(flow_y) * (y_pair[1] - y_pair[0])
                     + TURN_MAX * (head_pair[1] - head_pair[0]) + ACCEL_MAX * (speed_pair[1] - speed_pair[0]))
    return -jnp.maximum(value - damping, 0.0)


def reference(level_set, wind_field):
    d_theta = 2.0 * math.pi / NH
    d_speed = SPEED_SPAN / NV
    angles = jnp.arange(NH, dtype=jnp.int32).astype(jnp.float32) * d_theta
    cos_head = jnp.cos(angles)
    sin_head = jnp.sin(angles)
    speeds = SPEED_LOW + SPEED_SPAN * (jnp.arange(NV, dtype=jnp.int32).astype(jnp.float32) + 0.5) / NV
    rows_all = jnp.arange(NX, dtype=jnp.int32)

    def plane_max(position):
        winds = lax.dynamic_slice_in_dim(wind_field, position, 1, 1)
        return jnp.max(cell_rates(cos_head, sin_head, speeds, winds[0], winds[1], d_theta, d_speed))

    time_step = CFL_NUMBER / jnp.max(lax.map(plane_max, rows_all))

    def advance(surface):
        x_padded = extend(surface, 0)

        def one_plane(position):
            x_plane = lax.dynamic_slice_in_dim(surface, position, 1, 0)
            x_shifted = [lax.dynamic_slice_in_dim(x_padded, position + 3 + displace, 1, 0) for displace in range(-3, 4)]
            y_padded = extend(x_plane, 1)
            y_shifted = [y_padded[:, 3 + displace:3 + displace + NY] for displace in range(-3, 4)]
            head_padded = jnp.concatenate([x_plane[:, :, NH - 3:], x_plane, x_plane[:, :, :3]], axis=2)
            head_shifted = [head_padded[:, :, 3 + displace:3 + displace + NH] for displace in range(-3, 4)]
            winds = lax.dynamic_slice_in_dim(wind_field, position, 1, 1)
            return hamilton(weno_pair(x_shifted, CELL_SIZE), weno_pair(y_shifted, CELL_SIZE),
                            weno_pair(head_shifted, d_theta), weno_pair(speed_shifts(x_plane), d_speed),
                            cos_head, sin_head, speeds, winds[0], winds[1])

        return lax.map(one_plane, rows_all).reshape(surface.shape)

    section_one = level_set + time_step * advance(level_set)
    section_two = 0.75 * level_set + 0.25 * (section_one + time_step * advance(section_one))
    advanced = (1.0 / 3.0) * level_set + (2.0 / 3.0) * (section_two + time_step * advance(section_two))
    return advanced - level_set
```

```python
import functools
import math

import jax
import jax.numpy as jnp
import numpy as np
from jax import lax
from jax.experimental import pallas as pl
from jax.experimental.pallas import tpu as pltpu
from jax.sharding import PartitionSpec as P

CELL_SIZE = 0.05
SPEED_LOW = 0.1
SPEED_SPAN = 0.4
TURN_MAX = 1.0
ACCEL_MAX = 0.05
CFL_NUMBER = 0.5
WENO_EPS = 1e-06
SCALE = 32.0
PAD = 8
MESH = pl.DeviceIdType.MESH


def rcp(d):
    return pl.reciprocal(d, approx=False)


def eps_of(spacing):
    return 0.75 * WENO_EPS * (spacing * SCALE) ** 2


def smooth(d2, d3, e1, e2, e3, eps):
    g2 = 0.75 * d2
    g3 = 0.75 * d3
    c3 = g3 * d3 + eps
    s1 = e1 * (e1 + g2) + (g2 * d2 + eps)
    s2 = e2 * (e2 - g3) + c3
    s3 = e3 * (e3 - g3) + c3
    return s1, s2, s3


def upwind(dm2, dm1, d0, dp1, dp2, c0, c1, fh, eps):
    pos = fh > 0.0
    d1 = jnp.where(pos, dp2, dm2)
    d2 = jnp.where(pos, dp1, dm1)
    d4 = jnp.where(pos, dm1, dp1)
    c = jnp.where(pos, c1, c0)
    d3 = d0
    e1 = d2 - d1
    e2 = d3 - d2
    e3 = d4 - d3
    s1, s2, s3 = smooth(d2, d3, e1, e2, e3, eps)
    t1 = s2 * s3
    t2 = s1 * s3
    t3 = s1 * s2
    r1 = t1 * t1
    r2 = t2 * t2
    w3 = 1.5 * (t3 * t3)
    num = r1 * (e1 - e2) + w3 * (e2 - e3)
    den = (r1 + 6.0 * r2) + (w3 + w3)
    q = (d3 + 0.5 * d2) + num * rcp(den)
    return q * (jnp.abs(fh) * (1.0 / 3.0)) - c * fh


def triple(da, db, eps):
    e = db - da
    s2 = e * e + (0.75 * (da * db) + eps)
    h = 1.5 * e
    return e, s2 + db * h, s2, s2 - da * h


def face_pair(c, d2, d3, e1, e2, e3, s1, s2, s3):
    t1 = s2 * s3
    t2 = s1 * s3
    t3 = s1 * s2
    r1 = t1 * t1
    r2 = t2 * t2
    r3 = t3 * t3
    a = r1 * (e1 - e2)
    b = r3 * (e2 - e3)
    m = 6.0 * r2 + (r1 + r3)
    n = a + b
    left = (3.0 * c + (d3 + 0.5 * d2)) + (n + 0.5 * b) * rcp(m + (r3 + r3))
    right = ((d2 + 0.5 * d3) - 3.0 * c) + (n + 0.5 * a) * rcp(m + (r1 + r1))
    return left, right


def head_chunks(nh):
    return ((0, 3), (nh - 3, 3), (3, nh - 6))


def plane_chunks(nx):
    half = nx // 2
    return ((0, half), (half, nx - half))


def n_copies(nx, nh, tiles):
    return 2 * tiles * len(plane_chunks(nx)) + 2 * len(head_chunks(nh)) * (tiles + 1)


def kernel(sizes, axes, u_ref, wind_ref, flow_ref, rate_ref, out_hbm,
           b0, b1, b2, acc, rights, out_ref, va, vb, wind, best, peers, step,
           sends, recvs, rsend, rrecv, osem):
    nx, ny, nh, nv = sizes
    ngx, ngy, nha = axes
    bufs = (b0, b1, b2)
    d_theta = 2.0 * math.pi / (nh * nha)
    d_speed = SPEED_SPAN / nv
    tiles = ny // 8
    group = nh // 2
    heads, planes = head_chunks(nh), plane_chunks(nx)
    gx, gy, ha = lax.axis_index("gx"), lax.axis_index("gy"), lax.axis_index("ha")
    n_xy = ngx * ngy
    me = gx * ngy + gy

    def peer(delta):
        other = lax.rem(me + delta, n_xy)
        return {"gx": other // ngy, "gy": lax.rem(other, ngy)}

    up_ha = {"ha": lax.rem(ha + 1, nha)}
    down_ha = {"ha": lax.rem(ha + nha - 1, nha)}
    barrier = pltpu.get_barrier_semaphore()
    for delta in range(1, n_xy):
        pl.semaphore_signal(barrier, inc=1, device_id=peer(delta), device_id_type=MESH)
    for target in (up_ha, down_ha):
        pl.semaphore_signal(barrier, inc=1, device_id=target, device_id_type=MESH)

    def load_plane(x, carry):
        for k in range(nh):
            b0[3 + x, 3 + k, PAD:PAD + ny, :] = u_ref[x, k] * SCALE
        for comp in range(2):
            for y in range(ny):
                wind[comp, x, y:y + 1, :] = jnp.full((1, nv), wind_ref[comp, x, y] * (1.0 / CELL_SIZE), jnp.float32)
        return carry

    lax.fori_loop(0, nx, load_plane, 0)

    def rate_plane(x, top):
        for r in range(rate_ref.shape[1]):
            for t in range(tiles):
                fx = rate_ref[0, r:r + 1, :] + wind[0, x, 8 * t:8 * t + 8, :]
                fy = rate_ref[1, r:r + 1, :] + wind[1, x, 8 * t:8 * t + 8, :]
                top = jnp.maximum(top, jnp.abs(fx) + jnp.abs(fy))
        return top

    best[...] = lax.fori_loop(0, nx, rate_plane, jnp.zeros((8, 128), jnp.float32))

    pl.semaphore_wait(barrier, n_xy + 1)

    def tile_rows(t):
        return pl.ds(PAD + 8 * t, 8)

    def copies(s):
        buf = bufs[s]
        plans = {}
        for t in range(tiles):
            ys = tile_rows(t)
            for c, (x0, count) in enumerate(planes):
                xs = pl.ds(3 + x0, count)
                plans["h", t, c] = (
                    (buf.at[xs, pl.ds(nh, 3), ys], buf.at[xs, pl.ds(0, 3), ys], up_ha, None, None),
                    (buf.at[xs, pl.ds(3, 3), ys], buf.at[xs, pl.ds(3 + nh, 3), ys], down_ha, None, None),
                )
            for c, (k0, count) in enumerate(heads):
                hc = pl.ds(3 + k0, count)
                plans["x", t, c] = (
                    (buf.at[pl.ds(nx, 3), hc, ys], buf.at[pl.ds(0, 3), hc, ys], {"gx": gx + 1},
                     gx < ngx - 1, gx > 0),
                    (buf.at[pl.ds(3, 3), hc, ys], buf.at[pl.ds(3 + nx, 3), hc, ys], {"gx": gx - 1},
                     gx > 0, gx < ngx - 1),
                )
        xs = pl.ds(3, nx)
        for c, (k0, count) in enumerate(heads):
            hc = pl.ds(3 + k0, count)
            plans["y", tiles - 1, c] = (
                (buf.at[xs, hc, pl.ds(ny, PAD)], buf.at[xs, hc, pl.ds(0, PAD)], {"gy": gy + 1},
                 gy < ngy - 1, gy > 0),
            )
            plans["y", 0, c] = plans.get(("y", 0, c), ()) + (
                (buf.at[xs, hc, pl.ds(PAD, PAD)], buf.at[xs, hc, pl.ds(PAD + ny, PAD)], {"gy": gy - 1},
                 gy > 0, gy < ngy - 1),
            )
        made, at = {}, 0
        for key, group_of in plans.items():
            row = []
            for src, dst, target, has_out, has_in in group_of:
                row.append((pltpu.make_async_remote_copy(
                    src_ref=src, dst_ref=dst, send_sem=sends.at[s, at], recv_sem=recvs.at[s, at],
                    device_id=target, device_id_type=MESH), has_out, has_in))
                at += 1
            made[key] = row
        return made

    def under(condition, act):
        if condition is None:
            act()
        else:
            pl.when(condition)(act)

    rate_copies = [
        pltpu.make_async_remote_copy(
            src_ref=best, dst_ref=peers.at[delta - 1], send_sem=rsend.at[delta - 1],
            recv_sem=rrecv.at[delta - 1], device_id=peer(delta), device_id_type=MESH)
        for delta in range(1, n_xy)
    ]
    plans = [copies(s) for s in range(3)]

    def send(s, *key):
        for copy, has_out, _ in plans[s].get(key, ()):
            under(has_out, copy.start)

    def wait_in(s, *key):
        for copy, _, has_in in plans[s].get(key, ()):
            under(has_in, copy.wait_recv)

    def v_pass(buf, t):
        eps = eps_of(d_speed)
        coef = ACCEL_MAX / (3.0 * d_speed)
        e4 = np.float32(np.float32(eps * eps) ** 2)
        lane = lax.broadcasted_iota(jnp.int32, (8, nv), 1)
        edge = lane == 0
        keep = jnp.where((lane == 0) | (lane == nv - 1), 0.0, 1.0)
        inner_lane = jnp.where(edge, 0.0, 1.0)
        rows, rows_acc = tile_rows(t), slice(8 * t, 8 * t + 8)

        def first(x, half):
            for j in range(group):
                u = buf[3 + x, 3 + half * group + j, rows, :]
                q = u - pltpu.roll(u, 1, 1)
                va[half, 0, j] = q
                va[half, 1, j] = ((pltpu.roll(u, nv - 1, 1) - u) - q) * keep

        def second(half):
            for j in range(group):
                q, d = va[half, 0, j], va[half, 1, j]
                vb[half, 0, j] = pltpu.roll(d, 2, 1)
                vb[half, 1, j] = pltpu.roll(d, 1, 1)
                vb[half, 2, j] = d
                vb[half, 3, j] = pltpu.roll(d, nv - 1, 1)
                vb[half, 4, j] = pltpu.roll(q, 1, 1)
                vb[half, 5, j] = q
                vb[half, 6, j] = pltpu.roll(q, nv - 1, 1)

        def third(x, half):
            for j in range(group):
                k = half * group + j
                d1, d2, d3, d4, qb, qc, qd = [vb[half, i, j] for i in range(7)]
                e1 = d2 - d1
                e2 = d3 - d2
                e3 = d4 - d3
                s1, s2, s3 = smooth(d2, d3, e1, e2, e3, eps)
                t1 = s2 * s3
                t2 = s1 * s3
                t3 = s1 * s2
                r1 = t1 * t1
                r2 = t2 * t2
                r3 = t3 * t3
                f12 = e1 - e2
                f23 = e2 - e3
                r2l = jnp.where(edge, r1, r2)
                r3l = jnp.where(edge, e4, r3)
                r2r = jnp.where(edge, r3, r2)
                r1r = jnp.where(edge, e4, r1)
                cl = jnp.where(edge, qd, qc)
                cr = jnp.where(edge, qb, qc)
                nl = r1 * (f12 * inner_lane) + 1.5 * (r3l * f23)
                nr = 1.5 * (r1r * f12) + r3 * (f23 * inner_lane)
                left = (3.0 * cl + (d3 + 0.5 * d2)) + nl * rcp(r1 + 6.0 * r2l + 3.0 * r3l)
                right = ((d2 + 0.5 * d3) - 3.0 * cr) + nr * rcp(3.0 * r1r + 6.0 * r2r + r3)
                acc[x, k, rows_acc, :] = coef * left
                rights[x, k, rows_acc, :] = coef * right

        first(0, 0)
        first(0, 1)
        second(0)

        def body(x, carry):
            after = jnp.minimum(x + 1, nx - 1)
            third(x, 0)
            second(1)
            first(after, 0)
            third(x, 1)
            second(0)
            first(after, 1)
            return carry

        lax.fori_loop(0, nx, body, 0)

    def h_pass(s, t):
        buf = bufs[s]
        eps = eps_of(d_theta)
        coef = TURN_MAX / (3.0 * d_theta)
        rows, rows_acc = tile_rows(t), pl.ds(8 * t, 8)

        def body(x, carry):
            u = [buf[3 + x, j, rows, :] for j in range(nh + 6)]
            q = [u[j + 1] - u[j] for j in range(nh + 5)]
            d = [q[j + 1] - q[j] for j in range(nh + 4)]
            tr = [triple(d[j], d[j + 1], eps) for j in range(nh + 3)]
            before = None
            for f in range(nh + 1):
                left, right = face_pair(
                    q[f + 2], d[f + 1], d[f + 2], tr[f][0], tr[f + 1][0], tr[f + 2][0],
                    tr[f][1], tr[f + 1][2], tr[f + 2][3])
                if before is not None:
                    acc[x, f - 1, rows_acc, :] += coef * jnp.minimum(before, right)
                before = left
            return carry

        for c, (x0, count) in enumerate(planes):
            wait_in(s, "h", t, c)
            lax.fori_loop(x0, x0 + count, body, 0)

    def flow_row(comp, k):
        return flow_ref[comp, pl.ds(ha * nh + k, 1), :]

    def y_pass(s, t):
        buf = bufs[s]
        eps = eps_of(CELL_SIZE)
        rows = slice(8 * t, 8 * t + 8)

        def body(x, carry):
            for k in range(nh):
                u = [buf[3 + x, 3 + k, PAD + 8 * t + j:PAD + 8 * t + j + 8, :] for j in range(-3, 4)]
                q = [u[j + 1] - u[j] for j in range(6)]
                d = [q[j + 1] - q[j] for j in range(5)]
                fh = flow_row(1, k) + wind[1, x, rows, :]
                along_v = jnp.minimum(acc[x, k, rows, :], pltpu.roll(rights[x, k, rows, :], nv - 1, 1))
                acc[x, k, rows, :] = along_v + upwind(*d, q[2], q[3], fh, eps)
            return carry

        for c in range(len(heads)):
            if t == 0:
                for copy, _, has_in in plans[s]["y", tiles - 1, c][:1]:
                    under(has_in, copy.wait_recv)
            if t == tiles - 1:
                for copy, _, has_in in plans[s]["y", 0, c][-1:]:
                    under(has_in, copy.wait_recv)
        lax.fori_loop(0, nx, body, 0)

    def out_copy(t, c):
        k0, count = heads[c]
        part = (pl.ds(0, nx), pl.ds(k0, count), pl.ds(8 * t, 8))
        return pltpu.make_async_copy(out_ref.at[part], out_hbm.at[part], osem.at[t, c])

    def x_pass(s, t):
        buf = bufs[s]
        eps = eps_of(CELL_SIZE)
        rows, rows_acc = tile_rows(t), pl.ds(8 * t, 8)

        def body(k, carry):
            row = flow_row(0, k)
            dt = step[...]
            u = [buf[j, 3 + k, rows, :] for j in range(nx + 6)]
            q = [u[j + 1] - u[j] for j in range(nx + 5)]
            d = [q[j + 1] - q[j] for j in range(nx + 4)]
            for x in range(nx):
                fh = row + wind[0, x, rows_acc, :]
                total = acc[x, k, rows_acc, :] + upwind(*d[x:x + 5], q[x + 2], q[x + 3], fh, eps)
                moved = u[x + 3] - dt * jnp.maximum(total, 0.0)
                if s == 0:
                    b1[3 + x, 3 + k, rows, :] = moved
                elif s == 1:
                    b2[3 + x, 3 + k, rows, :] = 0.75 * b0[3 + x, 3 + k, rows, :] + 0.25 * moved
                else:
                    out_ref[x, k, rows_acc, :] = (moved - b0[3 + x, 3 + k, rows, :]) * (2.0 / (3.0 * SCALE))
            return carry

        for c, (k0, count) in enumerate(heads):
            wait_in(s, "x", t, c)
            lax.fori_loop(k0, k0 + count, body, 0)
            if s < 2:
                send(s + 1, "x", t, c)
                send(s + 1, "y", t, c)
                if c == 1:
                    for p in range(len(planes)):
                        send(s + 1, "h", t, p)
            else:
                out_copy(t, c).start()

    def fill_x(buf, t):
        rows = tile_rows(t)

        def ends(low):
            def act():
                def body(k, carry):
                    edge = buf[3 if low else nx + 2, 3 + k, rows, :]
                    slope = edge - buf[4 if low else nx + 1, 3 + k, rows, :]
                    for r in range(1, 4):
                        buf[3 - r if low else nx + 2 + r, 3 + k, rows, :] = edge + r * slope
                    return carry
                lax.fori_loop(0, nh, body, 0)
            return act
        pl.when(gx == 0)(ends(True))
        pl.when(gx == ngx - 1)(ends(False))

    def fill_y(buf, t):
        index = lax.broadcasted_iota(jnp.int32, (8, nv), 0).astype(jnp.float32)

        def ends(low):
            reach = (8.0 - index) if low else (index + 1.0)
            at, near, to = (PAD, PAD + 1, 0) if low else (PAD + ny - 1, PAD + ny - 2, PAD + ny)

            def act():
                def body(x, carry):
                    for k in range(nh):
                        edge = buf[3 + x, 3 + k, at:at + 1, :]
                        slope = edge - buf[3 + x, 3 + k, near:near + 1, :]
                        buf[3 + x, 3 + k, to:to + 8, :] = edge + reach * slope
                    return carry
                lax.fori_loop(0, nx, body, 0)
            return act
        if t == 0:
            pl.when(gy == 0)(ends(True))
        if t == tiles - 1:
            pl.when(gy == ngy - 1)(ends(False))

    for t in range(tiles):
        for p in range(len(planes)):
            send(0, "h", t, p)
        for c in range(len(heads)):
            send(0, "x", t, c)
            send(0, "y", t, c)
        if t == 0:
            for copy in rate_copies:
                copy.start()
    v_pass(b0, 0)
    for s in range(3):
        fill_y(bufs[s], 0)
        fill_y(bufs[s], tiles - 1) if tiles > 1 else None
        y_pass(s, 0)
        for t in range(1, tiles):
            v_pass(bufs[s], t)
            y_pass(s, t)
        for t in range(tiles):
            fill_x(bufs[s], t)
            h_pass(s, t)
            if s == 0 and t == 0:
                for copy in rate_copies:
                    copy.wait_recv()
                top = best[...]
                for delta in range(1, n_xy):
                    top = jnp.maximum(top, peers[delta - 1])
                rate = jnp.max(top, axis=(0, 1), keepdims=True) + (TURN_MAX / d_theta + ACCEL_MAX / d_speed)
                step[...] = jnp.broadcast_to(CFL_NUMBER / rate, step.shape)
            x_pass(s, t)
            if s < 2 and t == 0:
                v_pass(bufs[s + 1], 0)

    for t in range(tiles):
        for c in range(len(heads)):
            out_copy(t, c).wait()
    for copy in rate_copies:
        copy.wait_send()
    for s in range(3):
        for row in plans[s].values():
            for copy, has_out, _ in row:
                under(has_out, copy.wait_send)


def tables(nv, n_head):
    speeds = (SPEED_LOW + SPEED_SPAN * (np.arange(nv, dtype=np.float32) + np.float32(0.5)) / nv).astype(np.float32)
    angles = np.arange(n_head, dtype=np.float32) * np.float32(2.0 * math.pi / n_head)
    turns = np.stack([np.cos(angles.astype(np.float64)), np.sin(angles.astype(np.float64))])
    flow = (turns[:, :, None] * speeds[None, None, :] / CELL_SIZE).astype(np.float32)
    ends = np.concatenate([flow[:, :, 0], flow[:, :, -1]], axis=1)
    rows = -(-ends.shape[1] // 128)
    ends = np.concatenate([ends, np.repeat(ends[:, :1], rows * 128 - ends.shape[1], axis=1)], axis=1)
    return flow, ends.reshape(2, rows, 128)


def solution(mesh):
    axes = (mesh.shape["gx"], mesh.shape["gy"], mesh.shape["ha"])

    def body(level_set, wind_field):
        nx, ny, nh, nv = level_set.shape
        flow, ends = tables(nv, nh * axes[2])
        n_xy = axes[0] * axes[1]
        tiles = ny // 8
        count = n_copies(nx, nh, tiles)
        state = pltpu.VMEM((nx + 6, nh + 6, ny + 2 * PAD, nv), jnp.float32)
        cells = pltpu.VMEM((nx, nh, ny, nv), jnp.float32)
        vmem = pl.BlockSpec(memory_space=pltpu.VMEM)
        increment = pl.pallas_call(
            functools.partial(kernel, (nx, ny, nh, nv), axes),
            out_shape=jax.ShapeDtypeStruct((nx, nh, ny, nv), jnp.float32),
            in_specs=[vmem, pl.BlockSpec(memory_space=pltpu.SMEM), vmem, vmem],
            out_specs=pl.BlockSpec(memory_space=pltpu.HBM),
            scratch_shapes=[
                state, state, state, cells, cells, cells,
                pltpu.VMEM((2, 2, nh // 2, 8, nv), jnp.float32),
                pltpu.VMEM((2, 7, nh // 2, 8, nv), jnp.float32),
                pltpu.VMEM((2, nx, ny, nv), jnp.float32),
                pltpu.VMEM((8, 128), jnp.float32),
                pltpu.VMEM((n_xy - 1, 8, 128), jnp.float32),
                pltpu.VMEM((8, nv), jnp.float32),
                pltpu.SemaphoreType.DMA((3, count)),
                pltpu.SemaphoreType.DMA((3, count)),
                pltpu.SemaphoreType.DMA((n_xy - 1,)),
                pltpu.SemaphoreType.DMA((n_xy - 1,)),
                pltpu.SemaphoreType.DMA((tiles, len(head_chunks(nh)))),
            ],
            compiler_params=pltpu.CompilerParams(
                collective_id=0, has_side_effects=True, vmem_limit_bytes=56 * 2**20
            ),
        )(level_set.transpose(0, 2, 1, 3), wind_field, jnp.asarray(flow), jnp.asarray(ends))
        return increment.transpose(0, 2, 1, 3)

    return jax.shard_map(
        body,
        mesh=mesh,
        in_specs=(P("gx", "gy", "ha", None), P(None, "gx", "gy")),
        out_specs=P("gx", "gy", "ha", None),
        check_vma=False,
    )
```

```python
import functools
import math

import jax
import jax.numpy as jnp
import numpy as np
from jax import lax
from jax.experimental import pallas as pl
from jax.experimental.pallas import tpu as pltpu
from jax.sharding import PartitionSpec as P

CELL_SIZE = 0.05
SPEED_LOW = 0.1
SPEED_SPAN = 0.4
TURN_MAX = 1.0
ACCEL_MAX = 0.05
CFL_NUMBER = 0.5
WENO_EPS = 1e-06
SCALE = 32.0
PAD = 8
MESH = pl.DeviceIdType.MESH


def rcp(d):
    return pl.reciprocal(d, approx=False)


def eps_of(spacing):
    return 0.75 * WENO_EPS * (spacing * SCALE) ** 2


def smooth(d2, d3, e1, e2, e3, eps):
    g2 = 0.75 * d2
    g3 = 0.75 * d3
    c3 = g3 * d3 + eps
    s1 = e1 * (e1 + g2) + (g2 * d2 + eps)
    s2 = e2 * (e2 - g3) + c3
    s3 = e3 * (e3 - g3) + c3
    return s1, s2, s3


def upwind(dm2, dm1, d0, dp1, dp2, c0, c1, fh, eps):
    pos = fh > 0.0
    d1 = jnp.where(pos, dp2, dm2)
    d2 = jnp.where(pos, dp1, dm1)
    d4 = jnp.where(pos, dm1, dp1)
    c = jnp.where(pos, c1, c0)
    d3 = d0
    e1 = d2 - d1
    e2 = d3 - d2
    e3 = d4 - d3
    s1, s2, s3 = smooth(d2, d3, e1, e2, e3, eps)
    t1 = s2 * s3
    t2 = s1 * s3
    t3 = s1 * s2
    r1 = t1 * t1
    r2 = t2 * t2
    w3 = 1.5 * (t3 * t3)
    num = r1 * (e1 - e2) + w3 * (e2 - e3)
    den = (r1 + 6.0 * r2) + (w3 + w3)
    q = (d3 + 0.5 * d2) + num * rcp(den)
    return q * (jnp.abs(fh) * (1.0 / 3.0)) - c * fh


def triple(da, db, eps):
    e = db - da
    s2 = e * e + (0.75 * (da * db) + eps)
    h = 1.5 * e
    return e, s2 + db * h, s2, s2 - da * h


def face_pair(c, d2, d3, e1, e2, e3, s1, s2, s3):
    t1 = s2 * s3
    t2 = s1 * s3
    t3 = s1 * s2
    r1 = t1 * t1
    r2 = t2 * t2
    r3 = t3 * t3
    a = r1 * (e1 - e2)
    b = r3 * (e2 - e3)
    m = 6.0 * r2 + (r1 + r3)
    n = a + b
    left = (3.0 * c + (d3 + 0.5 * d2)) + (n + 0.5 * b) * rcp(m + (r3 + r3))
    right = ((d2 + 0.5 * d3) - 3.0 * c) + (n + 0.5 * a) * rcp(m + (r1 + r1))
    return left, right


def head_chunks(nh):
    half = (nh - 6) // 2
    return ((0, 3), (nh - 3, 3), (3, half), (3 + half, nh - 6 - half))


RELAYED = (0, 2)


def folded(axes):
    return axes[0] == 4 and axes[1] == 2


def plane_chunks(nx):
    half = nx // 2
    return ((0, half), (half, nx - half))


def n_copies(nx, nh, tiles):
    return 2 * tiles * len(plane_chunks(nx)) + 2 * len(head_chunks(nh)) * (tiles + 1)


def kernel(sizes, axes, u_ref, wind_ref, flow_ref, rate_ref, out_hbm,
           b0, b1, b2, acc, rights, out_ref, va, vb, wind, best, peers, step, relay,
           sends, recvs, rsend, rrecv, osem, lsend, lrecv):
    nx, ny, nh, nv = sizes
    ngx, ngy, nha = axes
    bufs = (b0, b1, b2)
    d_theta = 2.0 * math.pi / (nh * nha)
    d_speed = SPEED_SPAN / nv
    tiles = ny // 8
    group = nh // 2
    heads, planes = head_chunks(nh), plane_chunks(nx)
    gx, gy, ha = lax.axis_index("gx"), lax.axis_index("gy"), lax.axis_index("ha")
    n_xy = ngx * ngy
    me = gx * ngy + gy

    def peer(delta):
        other = lax.rem(me + delta, n_xy)
        return {"gx": other // ngy, "gy": lax.rem(other, ngy)}

    up_ha = {"ha": lax.rem(ha + 1, nha)}
    down_ha = {"ha": lax.rem(ha + nha - 1, nha)}
    barrier = pltpu.get_barrier_semaphore()
    for delta in range(1, n_xy):
        pl.semaphore_signal(barrier, inc=1, device_id=peer(delta), device_id_type=MESH)
    for target in (up_ha, down_ha):
        pl.semaphore_signal(barrier, inc=1, device_id=target, device_id_type=MESH)

    def load_plane(x, carry):
        for k in range(nh):
            b0[3 + x, 3 + k, PAD:PAD + ny, :] = u_ref[x, k] * SCALE
        for comp in range(2):
            for y in range(ny):
                wind[comp, x, y:y + 1, :] = jnp.full((1, nv), wind_ref[comp, x, y] * (1.0 / CELL_SIZE), jnp.float32)
        return carry

    lax.fori_loop(0, nx, load_plane, 0)

    def rate_plane(x, top):
        for r in range(rate_ref.shape[1]):
            for t in range(tiles):
                fx = rate_ref[0, r:r + 1, :] + wind[0, x, 8 * t:8 * t + 8, :]
                fy = rate_ref[1, r:r + 1, :] + wind[1, x, 8 * t:8 * t + 8, :]
                top = jnp.maximum(top, jnp.abs(fx) + jnp.abs(fy))
        return top

    best[...] = lax.fori_loop(0, nx, rate_plane, jnp.zeros((8, 128), jnp.float32))

    pl.semaphore_wait(barrier, n_xy + 1)

    def tile_rows(t):
        return pl.ds(PAD + 8 * t, 8)

    bending = folded(axes)
    places = []

    def copies(s):
        buf = bufs[s]
        plans = {}
        for t in range(tiles):
            ys = tile_rows(t)
            for c, (x0, count) in enumerate(planes):
                xs = pl.ds(3 + x0, count)
                plans["h", t, c] = (
                    (buf.at[xs, pl.ds(nh, 3), ys], buf.at[xs, pl.ds(0, 3), ys], up_ha, None, None),
                    (buf.at[xs, pl.ds(3, 3), ys], buf.at[xs, pl.ds(3 + nh, 3), ys], down_ha, None, None),
                )
            for c, (k0, count) in enumerate(heads):
                hc = pl.ds(3 + k0, count)
                around = bending and c in RELAYED
                plans["x", t, c] = (
                    (buf.at[pl.ds(nx, 3), hc, ys], buf.at[pl.ds(0, 3), hc, ys], {"gx": gx + 1},
                     (gx == 0) | (gx == 2) if around else gx < ngx - 1, gx > 0),
                    (buf.at[pl.ds(3, 3), hc, ys], buf.at[pl.ds(3 + nx, 3), hc, ys], {"gx": gx - 1},
                     (gx == 1) | (gx == 3) if around else gx > 0, gx < ngx - 1),
                )
        xs = pl.ds(3, nx)
        for c, (k0, count) in enumerate(heads):
            hc = pl.ds(3 + k0, count)
            plans["y", tiles - 1, c] = (
                (buf.at[xs, hc, pl.ds(ny, PAD)], buf.at[xs, hc, pl.ds(0, PAD)], {"gy": gy + 1},
                 gy < ngy - 1, gy > 0),
            )
            plans["y", 0, c] = plans.get(("y", 0, c), ()) + (
                (buf.at[xs, hc, pl.ds(PAD, PAD)], buf.at[xs, hc, pl.ds(PAD + ny, PAD)], {"gy": gy - 1},
                 gy > 0, gy < ngy - 1),
            )
        made, at, starts = {}, 0, {}
        for key, group_of in plans.items():
            row = []
            starts[key] = at
            for src, dst, target, has_out, has_in in group_of:
                row.append((pltpu.make_async_remote_copy(
                    src_ref=src, dst_ref=dst, send_sem=sends.at[s, at], recv_sem=recvs.at[s, at],
                    device_id=target, device_id_type=MESH), has_out, has_in))
                at += 1
            made[key] = row
        places.append(starts)
        return made

    def under(condition, act):
        if condition is None:
            act()
        else:
            pl.when(condition)(act)

    rate_copies = [
        pltpu.make_async_remote_copy(
            src_ref=best, dst_ref=peers.at[delta - 1], send_sem=rsend.at[delta - 1],
            recv_sem=rrecv.at[delta - 1], device_id=peer(delta), device_id_type=MESH)
        for delta in range(1, n_xy)
    ]
    plans = [copies(s) for s in range(3)]

    built = {}

    def legs(s, t, c):
        if (s, t, c) in built:
            return built[s, t, c]
        buf = bufs[s]
        k0, count = heads[c]
        hc, ys = pl.ds(3 + k0, count), tile_rows(t)
        held = relay.at[s, pl.ds(0, 3), pl.ds(k0, count), pl.ds(8 * t, 8)]
        i = RELAYED.index(c)
        rows = []
        for way, (src, dst, origin, middle, end) in enumerate((
            (buf.at[pl.ds(nx, 3), hc, ys], buf.at[pl.ds(0, 3), hc, ys], 1, 3, 2),
            (buf.at[pl.ds(3, 3), hc, ys], buf.at[pl.ds(3 + nx, 3), hc, ys], 2, 0, 1),
        )):
            out = pltpu.make_async_remote_copy(
                src_ref=src, dst_ref=held, send_sem=lsend.at[s, t, i, way], recv_sem=lrecv.at[s, t, i, way],
                device_id={"gx": middle}, device_id_type=MESH)
            on = pltpu.make_async_remote_copy(
                src_ref=held, dst_ref=dst, send_sem=sends.at[s, places[s]["x", t, c] + way],
                recv_sem=recvs.at[s, places[s]["x", t, c] + way],
                device_id={"gx": end}, device_id_type=MESH)
            rows.append((out, on, gx == origin, gx == middle))
        built[s, t, c] = rows
        return rows

    def forward(s, t):
        if bending:
            for c in RELAYED:
                for out, on, _, here in legs(s, t, c):
                    @pl.when(here)
                    def _():
                        out.wait_recv()
                        on.start()

    def send(s, *key):
        if bending and key[0] == "x" and key[2] in RELAYED:
            for out, _, from_here, _ in legs(s, *key[1:]):
                under(from_here, out.start)
        for copy, has_out, _ in plans[s].get(key, ()):
            under(has_out, copy.start)

    def wait_in(s, *key):
        for copy, _, has_in in plans[s].get(key, ()):
            under(has_in, copy.wait_recv)

    def v_pass(buf, t):
        eps = eps_of(d_speed)
        coef = ACCEL_MAX / (3.0 * d_speed)
        e4 = np.float32(np.float32(eps * eps) ** 2)
        lane = lax.broadcasted_iota(jnp.int32, (8, nv), 1)
        edge = lane == 0
        keep = jnp.where((lane == 0) | (lane == nv - 1), 0.0, 1.0)
        inner_lane = jnp.where(edge, 0.0, 1.0)
        rows, rows_acc = tile_rows(t), slice(8 * t, 8 * t + 8)

        def first(x, half):
            for j in range(group):
                u = buf[3 + x, 3 + half * group + j, rows, :]
                q = u - pltpu.roll(u, 1, 1)
                va[half, 0, j] = q
                va[half, 1, j] = ((pltpu.roll(u, nv - 1, 1) - u) - q) * keep

        def second(half):
            for j in range(group):
                q, d = va[half, 0, j], va[half, 1, j]
                vb[half, 0, j] = pltpu.roll(d, 2, 1)
                vb[half, 1, j] = pltpu.roll(d, 1, 1)
                vb[half, 2, j] = d
                vb[half, 3, j] = pltpu.roll(d, nv - 1, 1)
                vb[half, 4, j] = pltpu.roll(q, 1, 1)
                vb[half, 5, j] = q
                vb[half, 6, j] = pltpu.roll(q, nv - 1, 1)

        def third(x, half):
            for j in range(group):
                k = half * group + j
                d1, d2, d3, d4, qb, qc, qd = [vb[half, i, j] for i in range(7)]
                e1 = d2 - d1
                e2 = d3 - d2
                e3 = d4 - d3
                s1, s2, s3 = smooth(d2, d3, e1, e2, e3, eps)
                t1 = s2 * s3
                t2 = s1 * s3
                t3 = s1 * s2
                r1 = t1 * t1
                r2 = t2 * t2
                r3 = t3 * t3
                f12 = e1 - e2
                f23 = e2 - e3
                r2l = jnp.where(edge, r1, r2)
                r3l = jnp.where(edge, e4, r3)
                r2r = jnp.where(edge, r3, r2)
                r1r = jnp.where(edge, e4, r1)
                cl = jnp.where(edge, qd, qc)
                cr = jnp.where(edge, qb, qc)
                nl = r1 * (f12 * inner_lane) + 1.5 * (r3l * f23)
                nr = 1.5 * (r1r * f12) + r3 * (f23 * inner_lane)
                left = (3.0 * cl + (d3 + 0.5 * d2)) + nl * rcp(r1 + 6.0 * r2l + 3.0 * r3l)
                right = ((d2 + 0.5 * d3) - 3.0 * cr) + nr * rcp(3.0 * r1r + 6.0 * r2r + r3)
                acc[x, k, rows_acc, :] = coef * left
                rights[x, k, rows_acc, :] = coef * right

        first(0, 0)
        first(0, 1)
        second(0)

        def body(x, carry):
            after = jnp.minimum(x + 1, nx - 1)
            third(x, 0)
            second(1)
            first(after, 0)
            third(x, 1)
            second(0)
            first(after, 1)
            return carry

        lax.fori_loop(0, nx, body, 0)

    def h_pass(s, t):
        buf = bufs[s]
        eps = eps_of(d_theta)
        coef = TURN_MAX / (3.0 * d_theta)
        rows, rows_acc = tile_rows(t), pl.ds(8 * t, 8)

        def body(x, carry):
            u = [buf[3 + x, j, rows, :] for j in range(nh + 6)]
            q = [u[j + 1] - u[j] for j in range(nh + 5)]
            d = [q[j + 1] - q[j] for j in range(nh + 4)]
            tr = [triple(d[j], d[j + 1], eps) for j in range(nh + 3)]
            before = None
            for f in range(nh + 1):
                left, right = face_pair(
                    q[f + 2], d[f + 1], d[f + 2], tr[f][0], tr[f + 1][0], tr[f + 2][0],
                    tr[f][1], tr[f + 1][2], tr[f + 2][3])
                if before is not None:
                    acc[x, f - 1, rows_acc, :] += coef * jnp.minimum(before, right)
                before = left
            return carry

        for c, (x0, count) in enumerate(planes):
            wait_in(s, "h", t, c)
            lax.fori_loop(x0, x0 + count, body, 0)

    def flow_row(comp, k):
        return flow_ref[comp, pl.ds(ha * nh + k, 1), :]

    def y_pass(s, t):
        buf = bufs[s]
        eps = eps_of(CELL_SIZE)
        rows = slice(8 * t, 8 * t + 8)

        def body(x, carry):
            for k in range(nh):
                u = [buf[3 + x, 3 + k, PAD + 8 * t + j:PAD + 8 * t + j + 8, :] for j in range(-3, 4)]
                q = [u[j + 1] - u[j] for j in range(6)]
                d = [q[j + 1] - q[j] for j in range(5)]
                fh = flow_row(1, k) + wind[1, x, rows, :]
                along_v = jnp.minimum(acc[x, k, rows, :], pltpu.roll(rights[x, k, rows, :], nv - 1, 1))
                acc[x, k, rows, :] = along_v + upwind(*d, q[2], q[3], fh, eps)
            return carry

        for c in range(len(heads)):
            if t == 0:
                for copy, _, has_in in plans[s]["y", tiles - 1, c][:1]:
                    under(has_in, copy.wait_recv)
            if t == tiles - 1:
                for copy, _, has_in in plans[s]["y", 0, c][-1:]:
                    under(has_in, copy.wait_recv)
        lax.fori_loop(0, nx, body, 0)

    def out_copy(t, c):
        k0, count = heads[c]
        part = (pl.ds(0, nx), pl.ds(k0, count), pl.ds(8 * t, 8))
        return pltpu.make_async_copy(out_ref.at[part], out_hbm.at[part], osem.at[t, c])

    def x_pass(s, t):
        buf = bufs[s]
        eps = eps_of(CELL_SIZE)
        rows, rows_acc = tile_rows(t), pl.ds(8 * t, 8)

        def body(k, carry):
            row = flow_row(0, k)
            dt = step[...]
            u = [buf[j, 3 + k, rows, :] for j in range(nx + 6)]
            q = [u[j + 1] - u[j] for j in range(nx + 5)]
            d = [q[j + 1] - q[j] for j in range(nx + 4)]
            for x in range(nx):
                fh = row + wind[0, x, rows_acc, :]
                total = acc[x, k, rows_acc, :] + upwind(*d[x:x + 5], q[x + 2], q[x + 3], fh, eps)
                moved = u[x + 3] - dt * jnp.maximum(total, 0.0)
                if s == 0:
                    b1[3 + x, 3 + k, rows, :] = moved
                elif s == 1:
                    b2[3 + x, 3 + k, rows, :] = 0.75 * b0[3 + x, 3 + k, rows, :] + 0.25 * moved
                else:
                    out_ref[x, k, rows_acc, :] = (moved - b0[3 + x, 3 + k, rows, :]) * (2.0 / (3.0 * SCALE))
            return carry

        for c, (k0, count) in enumerate(heads):
            wait_in(s, "x", t, c)
            lax.fori_loop(k0, k0 + count, body, 0)
            if s < 2:
                send(s + 1, "x", t, c)
                send(s + 1, "y", t, c)
                if c == 1:
                    for p in range(len(planes)):
                        send(s + 1, "h", t, p)
            else:
                out_copy(t, c).start()

    def fill_x(buf, t):
        rows = tile_rows(t)

        def ends(low):
            def act():
                def body(k, carry):
                    edge = buf[3 if low else nx + 2, 3 + k, rows, :]
                    slope = edge - buf[4 if low else nx + 1, 3 + k, rows, :]
                    for r in range(1, 4):
                        buf[3 - r if low else nx + 2 + r, 3 + k, rows, :] = edge + r * slope
                    return carry
                lax.fori_loop(0, nh, body, 0)
            return act
        pl.when(gx == 0)(ends(True))
        pl.when(gx == ngx - 1)(ends(False))

    def fill_y(buf, t):
        index = lax.broadcasted_iota(jnp.int32, (8, nv), 0).astype(jnp.float32)

        def ends(low):
            reach = (8.0 - index) if low else (index + 1.0)
            at, near, to = (PAD, PAD + 1, 0) if low else (PAD + ny - 1, PAD + ny - 2, PAD + ny)

            def act():
                def body(x, carry):
                    for k in range(nh):
                        edge = buf[3 + x, 3 + k, at:at + 1, :]
                        slope = edge - buf[3 + x, 3 + k, near:near + 1, :]
                        buf[3 + x, 3 + k, to:to + 8, :] = edge + reach * slope
                    return carry
                lax.fori_loop(0, nx, body, 0)
            return act
        if t == 0:
            pl.when(gy == 0)(ends(True))
        if t == tiles - 1:
            pl.when(gy == ngy - 1)(ends(False))

    for t in range(tiles):
        for p in range(len(planes)):
            send(0, "h", t, p)
        for c in range(len(heads)):
            send(0, "x", t, c)
            send(0, "y", t, c)
        if t == 0:
            for copy in rate_copies:
                copy.start()
    v_pass(b0, 0)
    for s in range(3):
        fill_y(bufs[s], 0)
        fill_y(bufs[s], tiles - 1) if tiles > 1 else None
        y_pass(s, 0)
        for t in range(1, tiles):
            v_pass(bufs[s], t)
            if s == 0:
                forward(s, t - 1)
            y_pass(s, t)
        forward(s, tiles - 1)
        for t in range(tiles):
            fill_x(bufs[s], t)
            h_pass(s, t)
            if s == 0 and t == 0:
                for copy in rate_copies:
                    copy.wait_recv()
                top = best[...]
                for delta in range(1, n_xy):
                    top = jnp.maximum(top, peers[delta - 1])
                rate = jnp.max(top, axis=(0, 1), keepdims=True) + (TURN_MAX / d_theta + ACCEL_MAX / d_speed)
                step[...] = jnp.broadcast_to(CFL_NUMBER / rate, step.shape)
            x_pass(s, t)
            if s < 2 and t == 0:
                v_pass(bufs[s + 1], 0)
            if s < 2 and t > 0:
                forward(s + 1, t - 1)

    for t in range(tiles):
        for c in range(len(heads)):
            out_copy(t, c).wait()
    for copy in rate_copies:
        copy.wait_send()
    for s in range(3):
        for row in plans[s].values():
            for copy, has_out, _ in row:
                under(has_out, copy.wait_send)
        if bending:
            for t in range(tiles):
                for c in RELAYED:
                    for out, on, from_here, here in legs(s, t, c):
                        under(from_here, out.wait_send)
                        under(here, on.wait_send)


def tables(nv, n_head):
    speeds = (SPEED_LOW + SPEED_SPAN * (np.arange(nv, dtype=np.float32) + np.float32(0.5)) / nv).astype(np.float32)
    angles = np.arange(n_head, dtype=np.float32) * np.float32(2.0 * math.pi / n_head)
    turns = np.stack([np.cos(angles.astype(np.float64)), np.sin(angles.astype(np.float64))])
    flow = (turns[:, :, None] * speeds[None, None, :] / CELL_SIZE).astype(np.float32)
    ends = np.concatenate([flow[:, :, 0], flow[:, :, -1]], axis=1)
    rows = -(-ends.shape[1] // 128)
    ends = np.concatenate([ends, np.repeat(ends[:, :1], rows * 128 - ends.shape[1], axis=1)], axis=1)
    return flow, ends.reshape(2, rows, 128)


def solution(mesh):
    axes = (mesh.shape["gx"], mesh.shape["gy"], mesh.shape["ha"])

    def body(level_set, wind_field):
        nx, ny, nh, nv = level_set.shape
        flow, ends = tables(nv, nh * axes[2])
        n_xy = axes[0] * axes[1]
        tiles = ny // 8
        count = n_copies(nx, nh, tiles)
        state = pltpu.VMEM((nx + 6, nh + 6, ny + 2 * PAD, nv), jnp.float32)
        cells = pltpu.VMEM((nx, nh, ny, nv), jnp.float32)
        vmem = pl.BlockSpec(memory_space=pltpu.VMEM)
        increment = pl.pallas_call(
            functools.partial(kernel, (nx, ny, nh, nv), axes),
            out_shape=jax.ShapeDtypeStruct((nx, nh, ny, nv), jnp.float32),
            in_specs=[vmem, pl.BlockSpec(memory_space=pltpu.SMEM), vmem, vmem],
            out_specs=pl.BlockSpec(memory_space=pltpu.HBM),
            scratch_shapes=[
                state, state, state, cells, cells, cells,
                pltpu.VMEM((2, 2, nh // 2, 8, nv), jnp.float32),
                pltpu.VMEM((2, 7, nh // 2, 8, nv), jnp.float32),
                pltpu.VMEM((2, nx, ny, nv), jnp.float32),
                pltpu.VMEM((8, 128), jnp.float32),
                pltpu.VMEM((n_xy - 1, 8, 128), jnp.float32),
                pltpu.VMEM((8, nv), jnp.float32),
                pltpu.VMEM((3, 3, nh, ny, nv), jnp.float32),
                pltpu.SemaphoreType.DMA((3, count)),
                pltpu.SemaphoreType.DMA((3, count)),
                pltpu.SemaphoreType.DMA((n_xy - 1,)),
                pltpu.SemaphoreType.DMA((n_xy - 1,)),
                pltpu.SemaphoreType.DMA((tiles, len(head_chunks(nh)))),
                pltpu.SemaphoreType.DMA((3, tiles, len(RELAYED), 2)),
                pltpu.SemaphoreType.DMA((3, tiles, len(RELAYED), 2)),
            ],
            compiler_params=pltpu.CompilerParams(
                collective_id=0, has_side_effects=True, vmem_limit_bytes=56 * 2**20
            ),
        )(level_set.transpose(0, 2, 1, 3), wind_field, jnp.asarray(flow), jnp.asarray(ends))
        return increment.transpose(0, 2, 1, 3)

    return jax.shard_map(
        body,
        mesh=mesh,
        in_specs=(P("gx", "gy", "ha", None), P(None, "gx", "gy")),
        out_specs=P("gx", "gy", "ha", None),
        check_vma=False,
    )
```

```python
import functools
import math

import jax
import jax.numpy as jnp
import numpy as np
from jax import lax
from jax.experimental import pallas as pl
from jax.experimental.pallas import tpu as pltpu
from jax.sharding import PartitionSpec as P

CELL_SIZE = 0.05
SPEED_LOW = 0.1
SPEED_SPAN = 0.4
TURN_MAX = 1.0
ACCEL_MAX = 0.05
CFL_NUMBER = 0.5
WENO_EPS = 1e-06
SCALE = 32.0
PAD = 8
MESH = pl.DeviceIdType.MESH


def rcp(d):
    return pl.reciprocal(d, approx=False)


def eps_of(spacing):
    return 0.75 * WENO_EPS * (spacing * SCALE) ** 2


def smooth(d2, d3, e1, e2, e3, eps):
    g2 = 0.75 * d2
    g3 = 0.75 * d3
    c3 = g3 * d3 + eps
    s1 = e1 * (e1 + g2) + (g2 * d2 + eps)
    s2 = e2 * (e2 - g3) + c3
    s3 = e3 * (e3 - g3) + c3
    return s1, s2, s3


def upwind(dm2, dm1, d0, dp1, dp2, c0, c1, fh, eps):
    pos = fh > 0.0
    d1 = jnp.where(pos, dp2, dm2)
    d2 = jnp.where(pos, dp1, dm1)
    d4 = jnp.where(pos, dm1, dp1)
    c = jnp.where(pos, c1, c0)
    d3 = d0
    e1 = d2 - d1
    e2 = d3 - d2
    e3 = d4 - d3
    s1, s2, s3 = smooth(d2, d3, e1, e2, e3, eps)
    t1 = s2 * s3
    t2 = s1 * s3
    t3 = s1 * s2
    r1 = t1 * t1
    r2 = t2 * t2
    w3 = 1.5 * (t3 * t3)
    num = r1 * (e1 - e2) + w3 * (e2 - e3)
    den = (r1 + 6.0 * r2) + (w3 + w3)
    q = (d3 + 0.5 * d2) + num * rcp(den)
    return q * (jnp.abs(fh) * (1.0 / 3.0)) - c * fh


def triple(da, db, eps):
    e = db - da
    s2 = e * e + (0.75 * (da * db) + eps)
    h = 1.5 * e
    return e, s2 + db * h, s2, s2 - da * h


def face_pair(c, d2, d3, e1, e2, e3, s1, s2, s3):
    t1 = s2 * s3
    t2 = s1 * s3
    t3 = s1 * s2
    r1 = t1 * t1
    r2 = t2 * t2
    r3 = t3 * t3
    a = r1 * (e1 - e2)
    b = r3 * (e2 - e3)
    m = 6.0 * r2 + (r1 + r3)
    n = a + b
    left = (3.0 * c + (d3 + 0.5 * d2)) + (n + 0.5 * b) * rcp(m + (r3 + r3))
    right = ((d2 + 0.5 * d3) - 3.0 * c) + (n + 0.5 * a) * rcp(m + (r1 + r1))
    return left, right


def head_chunks(nh):
    half = (nh - 6) // 2
    return ((0, 3), (nh - 3, 3), (3, half), (3 + half, nh - 6 - half))


RELAYED = (0, 2)


def folded(axes):
    return axes[0] == 4 and axes[1] == 2 and axes[2] > 2


def plane_chunks(nx):
    half = nx // 2
    return ((0, half), (half, nx - half))


def n_copies(nx, nh, tiles):
    return 2 * tiles * len(plane_chunks(nx)) + 2 * len(head_chunks(nh)) * (tiles + 1)


def kernel(sizes, axes, u_hbm, wind_hbm, flow_hbm, rate_hbm, out_ref,
           b0, b1, b2, acc, rights, u_ref, wind_ref, flow_ref, rate_ref, va, vb, wind, best, peers, step, relay,
           sends, recvs, rsend, rrecv, isem, lsend, lrecv, far_x, low_in, high_in):
    nx, ny, nh, nv = sizes
    ngx, ngy, nha = axes
    bufs = (b0, b1, b2)
    d_theta = 2.0 * math.pi / (nh * nha)
    d_speed = SPEED_SPAN / nv
    tiles = ny // 8
    group = nh // 2
    heads, planes = head_chunks(nh), plane_chunks(nx)
    gx, gy, ha = lax.axis_index("gx"), lax.axis_index("gy"), lax.axis_index("ha")
    n_xy = ngx * ngy
    me = gx * ngy + gy

    def peer(delta):
        other = lax.rem(me + delta, n_xy)
        return {"gx": other // ngy, "gy": lax.rem(other, ngy)}

    up_ha = {"ha": lax.rem(ha + 1, nha)}
    down_ha = {"ha": lax.rem(ha + nha - 1, nha)}
    bending = folded(axes)
    beside, across = gx + 1 - 2 * lax.rem(gx, 2), lax.rem(gx + 2, 4)
    near = ({"gy": 1 - gy}, {"gx": beside}, {"gx": across},
            {"gx": beside, "gy": 1 - gy}, {"gx": across, "gy": 1 - gy})

    def under(condition, act):
        if condition is None:
            act()
        else:
            pl.when(condition)(act)

    def signal(semaphore, target):
        return lambda: pl.semaphore_signal(semaphore, inc=1, device_id=target, device_id_type=MESH)

    def await_one(semaphore):
        return lambda: pl.semaphore_wait(semaphore, 1)

    barrier = pltpu.get_barrier_semaphore()
    if bending:
        for target in near:
            signal(barrier, target)()
        under(ha < nha - 1, signal(barrier, {"ha": ha + 1}))
        under(ha > 0, signal(barrier, {"ha": ha - 1}))
    else:
        for delta in range(1, n_xy):
            signal(barrier, peer(delta))()
        for target in (up_ha, down_ha):
            signal(barrier, target)()

    fetches = [
        pltpu.make_async_copy(src, dst, isem.at[i])
        for i, (src, dst) in enumerate((
            (wind_hbm, wind_ref), (rate_hbm, rate_ref), (u_hbm, u_ref), (flow_hbm, flow_ref)))
    ]
    for fetch in fetches:
        fetch.start()
    for fetch in fetches:
        fetch.wait()

    def load_plane(x, carry):
        for k in range(nh):
            b0[3 + x, 3 + k, PAD:PAD + ny, :] = u_ref[x, k] * SCALE
        for comp in range(2):
            for y in range(ny):
                wind[comp, x, y:y + 1, :] = jnp.full((1, nv), wind_ref[comp, x, y] * (1.0 / CELL_SIZE), jnp.float32)
        return carry

    lax.fori_loop(0, nx, load_plane, 0)

    def rate_plane(x, top):
        for r in range(rate_ref.shape[1]):
            for t in range(tiles):
                fx = rate_ref[0, r:r + 1, :] + wind[0, x, 8 * t:8 * t + 8, :]
                fy = rate_ref[1, r:r + 1, :] + wind[1, x, 8 * t:8 * t + 8, :]
                top = jnp.maximum(top, jnp.abs(fx) + jnp.abs(fy))
        return top

    best[...] = lax.fori_loop(0, nx, rate_plane, jnp.zeros((8, 128), jnp.float32))

    if bending:
        beyond = (ha + nha - 2) // (nha - 1) + (2 * nha - 3 - ha) // (nha - 1)
        pl.semaphore_wait(barrier, len(near) + beyond)
    else:
        pl.semaphore_wait(barrier, n_xy + 1)

    def tile_rows(t):
        return pl.ds(PAD + 8 * t, 8)

    places = []

    def copies(s):
        buf = bufs[s]
        plans = {}
        for t in range(tiles):
            ys = tile_rows(t)
            for c, (x0, count) in enumerate(planes):
                xs = pl.ds(3 + x0, count)
                plans["h", t, c] = (
                    (buf.at[xs, pl.ds(nh, 3), ys], buf.at[xs, pl.ds(0, 3), ys], up_ha, None, None),
                    (buf.at[xs, pl.ds(3, 3), ys], buf.at[xs, pl.ds(3 + nh, 3), ys], down_ha, None, None),
                )
            for c, (k0, count) in enumerate(heads):
                hc = pl.ds(3 + k0, count)
                around = bending and c in RELAYED
                plans["x", t, c] = (
                    (buf.at[pl.ds(nx, 3), hc, ys], buf.at[pl.ds(0, 3), hc, ys], {"gx": gx + 1},
                     (gx == 0) | (gx == 2) if around else gx < ngx - 1, gx > 0),
                    (buf.at[pl.ds(3, 3), hc, ys], buf.at[pl.ds(3 + nx, 3), hc, ys], {"gx": gx - 1},
                     (gx == 1) | (gx == 3) if around else gx > 0, gx < ngx - 1),
                )
        xs = pl.ds(3, nx)
        for c, (k0, count) in enumerate(heads):
            hc = pl.ds(3 + k0, count)
            plans["y", tiles - 1, c] = (
                (buf.at[xs, hc, pl.ds(ny, PAD)], buf.at[xs, hc, pl.ds(0, PAD)], {"gy": gy + 1},
                 gy < ngy - 1, gy > 0),
            )
            plans["y", 0, c] = plans.get(("y", 0, c), ()) + (
                (buf.at[xs, hc, pl.ds(PAD, PAD)], buf.at[xs, hc, pl.ds(PAD + ny, PAD)], {"gy": gy - 1},
                 gy > 0, gy < ngy - 1),
            )
        made, at, starts = {}, 0, {}
        for key, group_of in plans.items():
            row = []
            starts[key] = at
            for src, dst, target, has_out, has_in in group_of:
                row.append((pltpu.make_async_remote_copy(
                    src_ref=src, dst_ref=dst, send_sem=sends.at[s, at], recv_sem=recvs.at[s, at],
                    device_id=target, device_id_type=MESH), has_out, has_in))
                at += 1
            made[key] = row
        places.append(starts)
        return made

    rate_copies = [
        pltpu.make_async_remote_copy(
            src_ref=best, dst_ref=peers.at[delta - 1], send_sem=rsend.at[delta - 1],
            recv_sem=rrecv.at[delta - 1], device_id=peer(delta), device_id_type=MESH)
        for delta in range(1, n_xy)
    ]

    def settle_rate():
        top = best[...]
        for i, copy in enumerate(rate_copies):
            copy.wait_recv()
            top = jnp.maximum(top, peers[i])
        rate = jnp.max(top, axis=(0, 1), keepdims=True) + (TURN_MAX / d_theta + ACCEL_MAX / d_speed)
        step[...] = jnp.broadcast_to(CFL_NUMBER / rate, step.shape)

    plans = [copies(s) for s in range(3)]

    built = {}

    def legs(s, t, c):
        if (s, t, c) in built:
            return built[s, t, c]
        buf = bufs[s]
        k0, count = heads[c]
        hc, ys = pl.ds(3 + k0, count), tile_rows(t)
        held = relay.at[s, pl.ds(0, 3), pl.ds(k0, count), pl.ds(8 * t, 8)]
        i = RELAYED.index(c)
        rows = []
        for way, (src, dst, origin, middle, end) in enumerate((
            (buf.at[pl.ds(nx, 3), hc, ys], buf.at[pl.ds(0, 3), hc, ys], 1, 3, 2),
            (buf.at[pl.ds(3, 3), hc, ys], buf.at[pl.ds(3 + nx, 3), hc, ys], 2, 0, 1),
        )):
            out = pltpu.make_async_remote_copy(
                src_ref=src, dst_ref=held, send_sem=lsend.at[s, t, i, way], recv_sem=lrecv.at[s, t, i, way],
                device_id={"gx": middle}, device_id_type=MESH)
            on = pltpu.make_async_remote_copy(
                src_ref=held, dst_ref=dst, send_sem=sends.at[s, places[s]["x", t, c] + way],
                recv_sem=recvs.at[s, places[s]["x", t, c] + way],
                device_id={"gx": end}, device_id_type=MESH)
            rows.append((out, on, gx == origin, gx == middle))
        built[s, t, c] = rows
        return rows

    def forward(s, t):
        if bending:
            for c in RELAYED:
                for out, on, _, here in legs(s, t, c):
                    @pl.when(here)
                    def _():
                        out.wait_recv()
                        on.start()

    def send(s, *key):
        if bending and key[0] == "x" and key[2] in RELAYED:
            for out, _, from_here, _ in legs(s, *key[1:]):
                under(from_here, out.start)
        for copy, has_out, _ in plans[s].get(key, ()):
            under(has_out, copy.start)

    def wait_in(s, *key):
        for copy, _, has_in in plans[s].get(key, ()):
            under(has_in, copy.wait_recv)

    def v_pass(buf, t):
        eps = eps_of(d_speed)
        coef = ACCEL_MAX / (3.0 * d_speed)
        e4 = np.float32(np.float32(eps * eps) ** 2)
        lane = lax.broadcasted_iota(jnp.int32, (8, nv), 1)
        edge = lane == 0
        keep = jnp.where((lane == 0) | (lane == nv - 1), 0.0, 1.0)
        inner_lane = jnp.where(edge, 0.0, 1.0)
        rows, rows_acc = tile_rows(t), slice(8 * t, 8 * t + 8)

        def first(x, half):
            for j in range(group):
                u = buf[3 + x, 3 + half * group + j, rows, :]
                q = u - pltpu.roll(u, 1, 1)
                va[half, 0, j] = q
                va[half, 1, j] = ((pltpu.roll(u, nv - 1, 1) - u) - q) * keep

        def second(half):
            for j in range(group):
                q, d = va[half, 0, j], va[half, 1, j]
                vb[half, 0, j] = pltpu.roll(d, 2, 1)
                vb[half, 1, j] = pltpu.roll(d, 1, 1)
                vb[half, 2, j] = d
                vb[half, 3, j] = pltpu.roll(d, nv - 1, 1)
                vb[half, 4, j] = pltpu.roll(q, 1, 1)
                vb[half, 5, j] = q
                vb[half, 6, j] = pltpu.roll(q, nv - 1, 1)

        def third(x, half):
            for j in range(group):
                k = half * group + j
                d1, d2, d3, d4, qb, qc, qd = [vb[half, i, j] for i in range(7)]
                e1 = d2 - d1
                e2 = d3 - d2
                e3 = d4 - d3
                s1, s2, s3 = smooth(d2, d3, e1, e2, e3, eps)
                t1 = s2 * s3
                t2 = s1 * s3
                t3 = s1 * s2
                r1 = t1 * t1
                r2 = t2 * t2
                r3 = t3 * t3
                f12 = e1 - e2
                f23 = e2 - e3
                r2l = jnp.where(edge, r1, r2)
                r3l = jnp.where(edge, e4, r3)
                r2r = jnp.where(edge, r3, r2)
                r1r = jnp.where(edge, e4, r1)
                cl = jnp.where(edge, qd, qc)
                cr = jnp.where(edge, qb, qc)
                nl = r1 * (f12 * inner_lane) + 1.5 * (r3l * f23)
                nr = 1.5 * (r1r * f12) + r3 * (f23 * inner_lane)
                left = (3.0 * cl + (d3 + 0.5 * d2)) + nl * rcp(r1 + 6.0 * r2l + 3.0 * r3l)
                right = ((d2 + 0.5 * d3) - 3.0 * cr) + nr * rcp(3.0 * r1r + 6.0 * r2r + r3)
                acc[x, k, rows_acc, :] = coef * left
                rights[x, k, rows_acc, :] = coef * right

        first(0, 0)
        first(0, 1)
        second(0)

        def body(x, carry):
            after = jnp.minimum(x + 1, nx - 1)
            third(x, 0)
            second(1)
            first(after, 0)
            third(x, 1)
            second(0)
            first(after, 1)
            return carry

        lax.fori_loop(0, nx, body, 0)

    def h_pass(s, t):
        buf = bufs[s]
        eps = eps_of(d_theta)
        coef = TURN_MAX / (3.0 * d_theta)
        rows, rows_acc = tile_rows(t), pl.ds(8 * t, 8)

        def body(x, carry):
            u = [buf[3 + x, j, rows, :] for j in range(nh + 6)]
            q = [u[j + 1] - u[j] for j in range(nh + 5)]
            d = [q[j + 1] - q[j] for j in range(nh + 4)]
            tr = [triple(d[j], d[j + 1], eps) for j in range(nh + 3)]
            before = None
            for f in range(nh + 1):
                left, right = face_pair(
                    q[f + 2], d[f + 1], d[f + 2], tr[f][0], tr[f + 1][0], tr[f + 2][0],
                    tr[f][1], tr[f + 1][2], tr[f + 2][3])
                if before is not None:
                    acc[x, f - 1, rows_acc, :] += coef * jnp.minimum(before, right)
                before = left
            return carry

        for c, (x0, count) in enumerate(planes):
            wait_in(s, "h", t, c)
            lax.fori_loop(x0, x0 + count, body, 0)

    def flow_row(comp, k):
        return flow_ref[comp, pl.ds(ha * nh + k, 1), :]

    def y_pass(s, t):
        buf = bufs[s]
        eps = eps_of(CELL_SIZE)
        rows = slice(8 * t, 8 * t + 8)

        def body(x, carry):
            for k in range(nh):
                u = [buf[3 + x, 3 + k, PAD + 8 * t + j:PAD + 8 * t + j + 8, :] for j in range(-3, 4)]
                q = [u[j + 1] - u[j] for j in range(6)]
                d = [q[j + 1] - q[j] for j in range(5)]
                fh = flow_row(1, k) + wind[1, x, rows, :]
                along_v = jnp.minimum(acc[x, k, rows, :], pltpu.roll(rights[x, k, rows, :], nv - 1, 1))
                acc[x, k, rows, :] = along_v + upwind(*d, q[2], q[3], fh, eps)
            return carry

        for c in range(len(heads)):
            if t == 0:
                for copy, _, has_in in plans[s]["y", tiles - 1, c][:1]:
                    under(has_in, copy.wait_recv)
            if t == tiles - 1:
                for copy, _, has_in in plans[s]["y", 0, c][-1:]:
                    under(has_in, copy.wait_recv)
        lax.fori_loop(0, nx, body, 0)

    def x_pass(s, t):
        buf = bufs[s]
        eps = eps_of(CELL_SIZE)
        rows, rows_acc = tile_rows(t), pl.ds(8 * t, 8)

        def body(k, carry):
            row = flow_row(0, k)
            dt = step[...]
            u = [buf[j, 3 + k, rows, :] for j in range(nx + 6)]
            q = [u[j + 1] - u[j] for j in range(nx + 5)]
            d = [q[j + 1] - q[j] for j in range(nx + 4)]
            for x in range(nx):
                fh = row + wind[0, x, rows_acc, :]
                total = acc[x, k, rows_acc, :] + upwind(*d[x:x + 5], q[x + 2], q[x + 3], fh, eps)
                moved = u[x + 3] - dt * jnp.maximum(total, 0.0)
                if s == 0:
                    b1[3 + x, 3 + k, rows, :] = moved
                elif s == 1:
                    b2[3 + x, 3 + k, rows, :] = 0.75 * b0[3 + x, 3 + k, rows, :] + 0.25 * moved
                else:
                    out_ref[x, k, rows_acc, :] = (moved - b0[3 + x, 3 + k, rows, :]) * (2.0 / (3.0 * SCALE))
            return carry

        for c, (k0, count) in enumerate(heads):
            wait_in(s, "x", t, c)
            lax.fori_loop(k0, k0 + count, body, 0)
            if s < 2:
                send(s + 1, "x", t, c)
                send(s + 1, "y", t, c)
                if c == 1:
                    for p in range(len(planes)):
                        send(s + 1, "h", t, p)

    def fill_x(buf, t):
        rows = tile_rows(t)

        def ends(low):
            def act():
                def body(k, carry):
                    edge = buf[3 if low else nx + 2, 3 + k, rows, :]
                    slope = edge - buf[4 if low else nx + 1, 3 + k, rows, :]
                    for r in range(1, 4):
                        buf[3 - r if low else nx + 2 + r, 3 + k, rows, :] = edge + r * slope
                    return carry
                lax.fori_loop(0, nh, body, 0)
            return act
        pl.when(gx == 0)(ends(True))
        pl.when(gx == ngx - 1)(ends(False))

    def fill_y(buf, t):
        index = lax.broadcasted_iota(jnp.int32, (8, nv), 0).astype(jnp.float32)

        def ends(low):
            reach = (8.0 - index) if low else (index + 1.0)
            at, near, to = (PAD, PAD + 1, 0) if low else (PAD + ny - 1, PAD + ny - 2, PAD + ny)

            def act():
                def body(x, carry):
                    for k in range(nh):
                        edge = buf[3 + x, 3 + k, at:at + 1, :]
                        slope = edge - buf[3 + x, 3 + k, near:near + 1, :]
                        buf[3 + x, 3 + k, to:to + 8, :] = edge + reach * slope
                    return carry
                lax.fori_loop(0, nx, body, 0)
            return act
        if t == 0:
            pl.when(gy == 0)(ends(True))
        if t == tiles - 1:
            pl.when(gy == ngy - 1)(ends(False))

    def open_x(t, far):
        for c in range(len(heads)):
            if far and c in RELAYED:
                continue
            for way, (copy, _, _) in enumerate(plans[0]["x", t, c]):
                under(gx == 1 + way if far else lax.rem(gx, 2) == way, copy.start)
            if c in RELAYED:
                for out, _, from_here, _ in legs(0, t, c):
                    under(from_here, out.start)

    def open_h(t, far):
        for p in range(len(planes)):
            for way, (copy, _, _) in enumerate(plans[0]["h", t, p]):
                edge = (nha - 1) * (1 - way)
                under(ha == edge if far else ha != edge, copy.start)

    def open_y(t):
        for c in range(len(heads)):
            send(0, "y", t, c)

    if bending:
        open_h(0, False)
        open_x(0, False)
        open_y(tiles - 1)
        signal(far_x, {"gx": beside})()
        under(ha == 1, signal(low_in, {"ha": ha + 1}))
        under(ha == nha - 2, signal(high_in, {"ha": ha - 1}))
        open_y(0) if tiles > 1 else None

        @pl.when((ha > 1) & (ha < nha - 1))
        def _():
            await_one(low_in)()
            signal(low_in, {"ha": ha + 1})()

        @pl.when((ha > 0) & (ha < nha - 2))
        def _():
            await_one(high_in)()
            signal(high_in, {"ha": ha - 1})()

        await_one(far_x)()
        open_x(0, True)
        for copy in rate_copies:
            copy.start()
        for t in range(1, tiles):
            open_x(t, False)
            open_x(t, True)
        v_pass(b0, 0)
        under(ha == nha - 1, await_one(low_in))
        under(ha == 0, await_one(high_in))
        open_h(0, True)
        for t in range(1, tiles):
            open_h(t, False)
            open_h(t, True)
    else:
        for t in range(tiles):
            for p in range(len(planes)):
                send(0, "h", t, p)
            for c in range(len(heads)):
                send(0, "x", t, c)
                send(0, "y", t, c)
        for copy in rate_copies:
            copy.start()
        v_pass(b0, 0)
    for s in range(3):
        fill_y(bufs[s], 0)
        fill_y(bufs[s], tiles - 1) if tiles > 1 else None
        y_pass(s, 0)
        for t in range(1, tiles):
            v_pass(bufs[s], t)
            if s == 0:
                forward(s, t - 1)
            y_pass(s, t)
        forward(s, tiles - 1)
        for t in range(tiles):
            fill_x(bufs[s], t)
            h_pass(s, t)
            if s == 0 and t == 0:
                settle_rate()
            x_pass(s, t)
            if s < 2 and t == 0:
                v_pass(bufs[s + 1], 0)
            if s < 2 and t > 0:
                forward(s + 1, t - 1)

    for copy in rate_copies:
        copy.wait_send()
    for s in range(3):
        for row in plans[s].values():
            for copy, has_out, _ in row:
                under(has_out, copy.wait_send)
        if bending:
            for t in range(tiles):
                for c in RELAYED:
                    for out, on, from_here, here in legs(s, t, c):
                        under(from_here, out.wait_send)
                        under(here, on.wait_send)


def tables(nv, n_head):
    speeds = (SPEED_LOW + SPEED_SPAN * (np.arange(nv, dtype=np.float32) + np.float32(0.5)) / nv).astype(np.float32)
    angles = np.arange(n_head, dtype=np.float32) * np.float32(2.0 * math.pi / n_head)
    turns = np.stack([np.cos(angles.astype(np.float64)), np.sin(angles.astype(np.float64))])
    flow = (turns[:, :, None] * speeds[None, None, :] / CELL_SIZE).astype(np.float32)
    ends = np.concatenate([flow[:, :, 0], flow[:, :, -1]], axis=1)
    rows = -(-ends.shape[1] // 128)
    ends = np.concatenate([ends, np.repeat(ends[:, :1], rows * 128 - ends.shape[1], axis=1)], axis=1)
    return flow, ends.reshape(2, rows, 128)


def solution(mesh):
    axes = (mesh.shape["gx"], mesh.shape["gy"], mesh.shape["ha"])

    def body(level_set, wind_field):
        nx, ny, nh, nv = level_set.shape
        flow, ends = tables(nv, nh * axes[2])
        n_xy = axes[0] * axes[1]
        tiles = ny // 8
        count = n_copies(nx, nh, tiles)
        state = pltpu.VMEM((nx + 6, nh + 6, ny + 2 * PAD, nv), jnp.float32)
        cells = pltpu.VMEM((nx, nh, ny, nv), jnp.float32)
        vmem = pl.BlockSpec(memory_space=pltpu.VMEM)
        increment = pl.pallas_call(
            functools.partial(kernel, (nx, ny, nh, nv), axes),
            out_shape=pltpu.VMEM((nx, nh, ny, nv), jnp.float32),
            in_specs=[pl.BlockSpec(memory_space=pltpu.HBM)] * 4,
            out_specs=vmem,
            scratch_shapes=[
                state, state, state, cells, cells, cells,
                pltpu.SMEM((2, nx, ny), jnp.float32),
                pltpu.VMEM(flow.shape, jnp.float32),
                pltpu.VMEM(ends.shape, jnp.float32),
                pltpu.VMEM((2, 2, nh // 2, 8, nv), jnp.float32),
                pltpu.VMEM((2, 7, nh // 2, 8, nv), jnp.float32),
                pltpu.VMEM((2, nx, ny, nv), jnp.float32),
                pltpu.VMEM((8, 128), jnp.float32),
                pltpu.VMEM((n_xy - 1, 8, 128), jnp.float32),
                pltpu.VMEM((8, nv), jnp.float32),
                pltpu.VMEM((3, 3, nh, ny, nv), jnp.float32),
                pltpu.SemaphoreType.DMA((3, count)),
                pltpu.SemaphoreType.DMA((3, count)),
                pltpu.SemaphoreType.DMA((n_xy - 1,)),
                pltpu.SemaphoreType.DMA((n_xy - 1,)),
                pltpu.SemaphoreType.DMA((4,)),
                pltpu.SemaphoreType.DMA((3, tiles, len(RELAYED), 2)),
                pltpu.SemaphoreType.DMA((3, tiles, len(RELAYED), 2)),
                pltpu.SemaphoreType.REGULAR,
                pltpu.SemaphoreType.REGULAR,
                pltpu.SemaphoreType.REGULAR,
            ],
            compiler_params=pltpu.CompilerParams(
                collective_id=0, has_side_effects=True, vmem_limit_bytes=56 * 2**20
            ),
        )(level_set.transpose(0, 2, 1, 3), wind_field, jnp.asarray(flow), jnp.asarray(ends))
        return increment.transpose(0, 2, 1, 3)

    return jax.shard_map(
        body,
        mesh=mesh,
        in_specs=(P("gx", "gy", "ha", None), P(None, "gx", "gy")),
        out_specs=P("gx", "gy", "ha", None),
        check_vma=False,
    )
```

```python
import functools
import math

import jax
import jax.numpy as jnp
import numpy as np
from jax import lax
from jax.experimental import pallas as pl
from jax.experimental.pallas import tpu as pltpu
from jax.sharding import PartitionSpec as P

CELL_SIZE = 0.05
SPEED_LOW = 0.1
SPEED_SPAN = 0.4
TURN_MAX = 1.0
ACCEL_MAX = 0.05
CFL_NUMBER = 0.5
WENO_EPS = 1e-06
SCALE = 32.0
PAD = 8
MESH = pl.DeviceIdType.MESH


def rcp(d):
    return pl.reciprocal(d, approx=False)


def eps_of(spacing):
    return 0.75 * WENO_EPS * (spacing * SCALE) ** 2


def smooth(d2, d3, e1, e2, e3, eps):
    g2 = 0.75 * d2
    g3 = 0.75 * d3
    c3 = g3 * d3 + eps
    s1 = e1 * (e1 + g2) + (g2 * d2 + eps)
    s2 = e2 * (e2 - g3) + c3
    s3 = e3 * (e3 - g3) + c3
    return s1, s2, s3


def upwind(dm2, dm1, d0, dp1, dp2, c0, c1, fh, eps):
    pos = fh > 0.0
    d1 = jnp.where(pos, dp2, dm2)
    d2 = jnp.where(pos, dp1, dm1)
    d4 = jnp.where(pos, dm1, dp1)
    c = jnp.where(pos, c1, c0)
    d3 = d0
    e1 = d2 - d1
    e2 = d3 - d2
    e3 = d4 - d3
    s1, s2, s3 = smooth(d2, d3, e1, e2, e3, eps)
    t1 = s2 * s3
    t2 = s1 * s3
    t3 = s1 * s2
    r1 = t1 * t1
    r2 = t2 * t2
    w3 = 1.5 * (t3 * t3)
    num = r1 * (e1 - e2) + w3 * (e2 - e3)
    den = (r1 + 6.0 * r2) + (w3 + w3)
    q = (d3 + 0.5 * d2) + num * rcp(den)
    return q * (jnp.abs(fh) * (1.0 / 3.0)) - c * fh


def triple(da, db, eps):
    e = db - da
    s2 = e * e + (0.75 * (da * db) + eps)
    h = 1.5 * e
    return e, s2 + db * h, s2, s2 - da * h


def face_pair(c, d2, d3, e1, e2, e3, s1, s2, s3):
    t1 = s2 * s3
    t2 = s1 * s3
    t3 = s1 * s2
    r1 = t1 * t1
    r2 = t2 * t2
    r3 = t3 * t3
    a = r1 * (e1 - e2)
    b = r3 * (e2 - e3)
    m = 6.0 * r2 + (r1 + r3)
    n = a + b
    left = (3.0 * c + (d3 + 0.5 * d2)) + (n + 0.5 * b) * rcp(m + (r3 + r3))
    right = ((d2 + 0.5 * d3) - 3.0 * c) + (n + 0.5 * a) * rcp(m + (r1 + r1))
    return left, right


def head_chunks(nh):
    half = nh // 2
    return ((0, half), (half, nh - half))


RELAYED = (1,)


def folded(axes):
    return axes[0] == 4 and axes[1] == 2 and axes[2] > 2


def plane_chunks(nx):
    half = nx // 2
    return ((0, half), (half, nx - half))


def n_copies(nx, nh, tiles):
    return 2 * len(plane_chunks(nx)) * (tiles + 1) + 2 * len(head_chunks(nh)) * tiles


def kernel(sizes, axes, u_hbm, wind_hbm, flow_hbm, rate_hbm, out_ref,
           b0, b1, b2, acc, rights, u_ref, wind_ref, flow_ref, rate_ref, va, vb, wind, best, peers, step, relay,
           sends, recvs, rsend, rrecv, isem, lsend, lrecv, far_x, low_in, high_in):
    nx, ny, nh, nv = sizes
    ngx, ngy, nha = axes
    bufs = (b0, b1, b2)
    d_theta = 2.0 * math.pi / (nh * nha)
    d_speed = SPEED_SPAN / nv
    tiles = ny // 8
    group = nh // 2
    heads, planes = head_chunks(nh), plane_chunks(nx)
    gx, gy, ha = lax.axis_index("gx"), lax.axis_index("gy"), lax.axis_index("ha")
    n_xy = ngx * ngy
    me = gx * ngy + gy

    def peer(delta):
        other = lax.rem(me + delta, n_xy)
        return {"gx": other // ngy, "gy": lax.rem(other, ngy)}

    up_ha = {"ha": lax.rem(ha + 1, nha)}
    down_ha = {"ha": lax.rem(ha + nha - 1, nha)}
    bending = folded(axes)
    beside, across = gx + 1 - 2 * lax.rem(gx, 2), lax.rem(gx + 2, 4)
    near = ({"gy": 1 - gy}, {"gx": beside}, {"gx": across},
            {"gx": beside, "gy": 1 - gy}, {"gx": across, "gy": 1 - gy})

    def under(condition, act):
        if condition is None:
            act()
        else:
            pl.when(condition)(act)

    def signal(semaphore, target):
        return lambda: pl.semaphore_signal(semaphore, inc=1, device_id=target, device_id_type=MESH)

    def await_one(semaphore):
        return lambda: pl.semaphore_wait(semaphore, 1)

    barrier = pltpu.get_barrier_semaphore()
    if bending:
        for target in near:
            signal(barrier, target)()
        under(ha < nha - 1, signal(barrier, {"ha": ha + 1}))
        under(ha > 0, signal(barrier, {"ha": ha - 1}))
    else:
        for delta in range(1, n_xy):
            signal(barrier, peer(delta))()
        for target in (up_ha, down_ha):
            signal(barrier, target)()

    fetches = [
        pltpu.make_async_copy(src, dst, isem.at[i])
        for i, (src, dst) in enumerate((
            (wind_hbm, wind_ref), (rate_hbm, rate_ref), (u_hbm, u_ref), (flow_hbm, flow_ref)))
    ]
    for fetch in fetches:
        fetch.start()
    for fetch in fetches:
        fetch.wait()

    def load_plane(x, carry):
        for k in range(nh):
            b0[3 + x, 3 + k, PAD:PAD + ny, :] = u_ref[x, k] * SCALE
        for comp in range(2):
            for y in range(ny):
                wind[comp, x, y:y + 1, :] = jnp.full((1, nv), wind_ref[comp, x, y] * (1.0 / CELL_SIZE), jnp.float32)
        return carry

    lax.fori_loop(0, nx, load_plane, 0)

    def rate_plane(x, top):
        for r in range(rate_ref.shape[1]):
            for t in range(tiles):
                fx = rate_ref[0, r:r + 1, :] + wind[0, x, 8 * t:8 * t + 8, :]
                fy = rate_ref[1, r:r + 1, :] + wind[1, x, 8 * t:8 * t + 8, :]
                top = jnp.maximum(top, jnp.abs(fx) + jnp.abs(fy))
        return top

    best[...] = lax.fori_loop(0, nx, rate_plane, jnp.zeros((8, 128), jnp.float32))

    if bending:
        beyond = (ha + nha - 2) // (nha - 1) + (2 * nha - 3 - ha) // (nha - 1)
        pl.semaphore_wait(barrier, len(near) + beyond)
    else:
        pl.semaphore_wait(barrier, n_xy + 1)

    def tile_rows(t):
        return pl.ds(PAD + 8 * t, 8)

    places = []

    def copies(s):
        buf = bufs[s]
        plans = {}
        for t in range(tiles):
            ys = tile_rows(t)
            for c, (x0, count) in enumerate(planes):
                xs = pl.ds(3 + x0, count)
                plans["h", t, c] = (
                    (buf.at[xs, pl.ds(nh, 3), ys], buf.at[xs, pl.ds(0, 3), ys], up_ha, None, None),
                    (buf.at[xs, pl.ds(3, 3), ys], buf.at[xs, pl.ds(3 + nh, 3), ys], down_ha, None, None),
                )
            for c, (k0, count) in enumerate(heads):
                hc = pl.ds(3 + k0, count)
                around = bending and c in RELAYED
                plans["x", t, c] = (
                    (buf.at[pl.ds(nx, 3), hc, ys], buf.at[pl.ds(0, 3), hc, ys], {"gx": gx + 1},
                     (gx == 0) | (gx == 2) if around else gx < ngx - 1, gx > 0),
                    (buf.at[pl.ds(3, 3), hc, ys], buf.at[pl.ds(3 + nx, 3), hc, ys], {"gx": gx - 1},
                     (gx == 1) | (gx == 3) if around else gx > 0, gx < ngx - 1),
                )
        hc = pl.ds(3, nh)
        for c, (x0, count) in enumerate(planes):
            xs = pl.ds(3 + x0, count)
            plans["y", tiles - 1, c] = (
                (buf.at[xs, hc, pl.ds(ny, PAD)], buf.at[xs, hc, pl.ds(0, PAD)], {"gy": gy + 1},
                 gy < ngy - 1, gy > 0),
            )
            plans["y", 0, c] = plans.get(("y", 0, c), ()) + (
                (buf.at[xs, hc, pl.ds(PAD, PAD)], buf.at[xs, hc, pl.ds(PAD + ny, PAD)], {"gy": gy - 1},
                 gy > 0, gy < ngy - 1),
            )
        made, at, starts = {}, 0, {}
        for key, group_of in plans.items():
            row = []
            starts[key] = at
            for src, dst, target, has_out, has_in in group_of:
                row.append((pltpu.make_async_remote_copy(
                    src_ref=src, dst_ref=dst, send_sem=sends.at[s, at], recv_sem=recvs.at[s, at],
                    device_id=target, device_id_type=MESH), has_out, has_in))
                at += 1
            made[key] = row
        places.append(starts)
        return made

    rate_copies = [
        pltpu.make_async_remote_copy(
            src_ref=best, dst_ref=peers.at[delta - 1], send_sem=rsend.at[delta - 1],
            recv_sem=rrecv.at[delta - 1], device_id=peer(delta), device_id_type=MESH)
        for delta in range(1, n_xy)
    ]

    def settle_rate():
        top = best[...]
        for i, copy in enumerate(rate_copies):
            copy.wait_recv()
            top = jnp.maximum(top, peers[i])
        rate = jnp.max(top, axis=(0, 1), keepdims=True) + (TURN_MAX / d_theta + ACCEL_MAX / d_speed)
        step[...] = jnp.broadcast_to(CFL_NUMBER / rate, step.shape)

    plans = [copies(s) for s in range(3)]

    built = {}

    def legs(s, t, c):
        if (s, t, c) in built:
            return built[s, t, c]
        buf = bufs[s]
        k0, count = heads[c]
        hc, ys = pl.ds(3 + k0, count), tile_rows(t)
        held = relay.at[s, pl.ds(0, 3), pl.ds(k0, count), pl.ds(8 * t, 8)]
        i = RELAYED.index(c)
        rows = []
        for way, (src, dst, origin, middle, end) in enumerate((
            (buf.at[pl.ds(nx, 3), hc, ys], buf.at[pl.ds(0, 3), hc, ys], 1, 3, 2),
            (buf.at[pl.ds(3, 3), hc, ys], buf.at[pl.ds(3 + nx, 3), hc, ys], 2, 0, 1),
        )):
            out = pltpu.make_async_remote_copy(
                src_ref=src, dst_ref=held, send_sem=lsend.at[s, t, i, way], recv_sem=lrecv.at[s, t, i, way],
                device_id={"gx": middle}, device_id_type=MESH)
            on = pltpu.make_async_remote_copy(
                src_ref=held, dst_ref=dst, send_sem=sends.at[s, places[s]["x", t, c] + way],
                recv_sem=recvs.at[s, places[s]["x", t, c] + way],
                device_id={"gx": end}, device_id_type=MESH)
            rows.append((out, on, gx == origin, gx == middle))
        built[s, t, c] = rows
        return rows

    def forward(s, t):
        if bending:
            for c in RELAYED:
                for out, on, _, here in legs(s, t, c):
                    @pl.when(here)
                    def _():
                        out.wait_recv()
                        on.start()

    def send(s, *key):
        for copy, has_out, _ in plans[s].get(key, ()):
            under(has_out, copy.start)

    def send_x(s, t, way):
        for c in range(len(heads)):
            copy, has_out, _ = plans[s]["x", t, c][way]
            under(has_out, copy.start)
            if bending and c in RELAYED:
                out, _, from_here, _ = legs(s, t, c)[way]
                under(from_here, out.start)

    def wait_in(s, *key):
        for copy, _, has_in in plans[s].get(key, ()):
            under(has_in, copy.wait_recv)

    def v_parts(buf, t):
        eps = eps_of(d_speed)
        coef = ACCEL_MAX / (3.0 * d_speed)
        e4 = np.float32(np.float32(eps * eps) ** 2)
        lane = lax.broadcasted_iota(jnp.int32, (8, nv), 1)
        edge = lane == 0
        keep = jnp.where((lane == 0) | (lane == nv - 1), 0.0, 1.0)
        inner_lane = jnp.where(edge, 0.0, 1.0)
        rows, rows_acc = tile_rows(t), slice(8 * t, 8 * t + 8)

        def first(x, half):
            for j in range(group):
                u = buf[3 + x, 3 + half * group + j, rows, :]
                q = u - pltpu.roll(u, 1, 1)
                va[half, 0, j] = q
                va[half, 1, j] = ((pltpu.roll(u, nv - 1, 1) - u) - q) * keep

        def second(half):
            for j in range(group):
                q, d = va[half, 0, j], va[half, 1, j]
                vb[half, 0, j] = pltpu.roll(d, 2, 1)
                vb[half, 1, j] = pltpu.roll(d, 1, 1)
                vb[half, 2, j] = d
                vb[half, 3, j] = pltpu.roll(d, nv - 1, 1)
                vb[half, 4, j] = pltpu.roll(q, 1, 1)
                vb[half, 5, j] = q
                vb[half, 6, j] = pltpu.roll(q, nv - 1, 1)

        def third(x, half):
            for j in range(group):
                k = half * group + j
                d1, d2, d3, d4, qb, qc, qd = [vb[half, i, j] for i in range(7)]
                e1 = d2 - d1
                e2 = d3 - d2
                e3 = d4 - d3
                s1, s2, s3 = smooth(d2, d3, e1, e2, e3, eps)
                t1 = s2 * s3
                t2 = s1 * s3
                t3 = s1 * s2
                r1 = t1 * t1
                r2 = t2 * t2
                r3 = t3 * t3
                f12 = e1 - e2
                f23 = e2 - e3
                r2l = jnp.where(edge, r1, r2)
                r3l = jnp.where(edge, e4, r3)
                r2r = jnp.where(edge, r3, r2)
                r1r = jnp.where(edge, e4, r1)
                cl = jnp.where(edge, qd, qc)
                cr = jnp.where(edge, qb, qc)
                nl = r1 * (f12 * inner_lane) + 1.5 * (r3l * f23)
                nr = 1.5 * (r1r * f12) + r3 * (f23 * inner_lane)
                left = (3.0 * cl + (d3 + 0.5 * d2)) + nl * rcp(r1 + 6.0 * r2l + 3.0 * r3l)
                right = ((d2 + 0.5 * d3) - 3.0 * cr) + nr * rcp(3.0 * r1r + 6.0 * r2r + r3)
                acc[x, k, rows_acc, :] = coef * left
                rights[x, k, rows_acc, :] = coef * right

        def begin():
            first(0, 0)
            first(0, 1)
            second(0)

        def body(x, carry):
            after = jnp.minimum(x + 1, nx - 1)
            third(x, 0)
            second(1)
            first(after, 0)
            third(x, 1)
            second(0)
            first(after, 1)
            return carry

        return begin, body

    def v_pass(buf, t):
        begin, body = v_parts(buf, t)
        begin()
        lax.fori_loop(0, nx, body, 0)

    def h_pass(s, t):
        buf = bufs[s]
        eps = eps_of(d_theta)
        coef = TURN_MAX / (3.0 * d_theta)
        rows, rows_acc = tile_rows(t), pl.ds(8 * t, 8)

        def body(x, carry):
            dt = step[...]
            u = [buf[3 + x, j, rows, :] for j in range(nh + 6)]
            q = [u[j + 1] - u[j] for j in range(nh + 5)]
            d = [q[j + 1] - q[j] for j in range(nh + 4)]
            tr = [triple(d[j], d[j + 1], eps) for j in range(nh + 3)]
            before = None
            for f in range(nh + 1):
                left, right = face_pair(
                    q[f + 2], d[f + 1], d[f + 2], tr[f][0], tr[f + 1][0], tr[f + 2][0],
                    tr[f][1], tr[f + 1][2], tr[f + 2][3])
                if before is not None:
                    k = f - 1
                    total = acc[x, k, rows_acc, :] + coef * jnp.minimum(before, right)
                    moved = u[k + 3] - dt * jnp.maximum(total, 0.0)
                    if s == 0:
                        b1[3 + x, 3 + k, rows, :] = moved
                    elif s == 1:
                        b2[3 + x, 3 + k, rows, :] = 0.75 * b0[3 + x, 3 + k, rows, :] + 0.25 * moved
                    else:
                        out_ref[x, k, rows_acc, :] = (moved - b0[3 + x, 3 + k, rows, :]) * (2.0 / (3.0 * SCALE))
                before = left
            return carry

        for c, (x0, count) in enumerate(planes):
            wait_in(s, "h", t, c)
            lax.fori_loop(x0, x0 + count, body, 0)
            if s < 2:
                send(s + 1, "h", t, c)
                if c == 0:
                    send_x(s + 1, t, 1)
                if c == len(planes) - 1:
                    send_x(s + 1, t, 0)
                send(s + 1, "y", t, c)

    def flow_row(comp, k):
        return flow_ref[comp, pl.ds(ha * nh + k, 1), :]

    def y_parts(s, t):
        buf = bufs[s]
        eps = eps_of(CELL_SIZE)
        rows = slice(8 * t, 8 * t + 8)

        def begin():
            for c in range(len(planes)):
                if t == 0:
                    for copy, _, has_in in plans[s]["y", tiles - 1, c][:1]:
                        under(has_in, copy.wait_recv)
                if t == tiles - 1:
                    for copy, _, has_in in plans[s]["y", 0, c][-1:]:
                        under(has_in, copy.wait_recv)

        def body(x, carry):
            for k in range(nh):
                u = [buf[3 + x, 3 + k, PAD + 8 * t + j:PAD + 8 * t + j + 8, :] for j in range(-3, 4)]
                q = [u[j + 1] - u[j] for j in range(6)]
                d = [q[j + 1] - q[j] for j in range(5)]
                fh = flow_row(1, k) + wind[1, x, rows, :]
                along_v = jnp.minimum(acc[x, k, rows, :], pltpu.roll(rights[x, k, rows, :], nv - 1, 1))
                acc[x, k, rows, :] = along_v + upwind(*d, q[2], q[3], fh, eps)
            return carry

        return begin, body

    def y_pass(s, t):
        begin, body = y_parts(s, t)
        begin()
        lax.fori_loop(0, nx, body, 0)

    def yv_pass(s, t):
        y_begin, y_body = y_parts(s, t)
        v_begin, v_body = v_parts(bufs[s], t + 1)
        v_begin()
        y_begin()

        def body(x, carry):
            y_body(x, carry)
            v_body(x, carry)
            return carry

        lax.fori_loop(0, nx, body, 0)

    def x_pass(s, t):
        buf = bufs[s]
        eps = eps_of(CELL_SIZE)
        rows, rows_acc = tile_rows(t), pl.ds(8 * t, 8)

        def body(k, carry):
            row = flow_row(0, k)
            u = [buf[j, 3 + k, rows, :] for j in range(nx + 6)]
            q = [u[j + 1] - u[j] for j in range(nx + 5)]
            d = [q[j + 1] - q[j] for j in range(nx + 4)]
            for x in range(nx):
                fh = row + wind[0, x, rows_acc, :]
                acc[x, k, rows_acc, :] += upwind(*d[x:x + 5], q[x + 2], q[x + 3], fh, eps)
            return carry

        for c, (k0, count) in enumerate(heads):
            wait_in(s, "x", t, c)
            lax.fori_loop(k0, k0 + count, body, 0)

    def fill_x(buf, t):
        rows = tile_rows(t)

        def ends(low):
            def act():
                def body(k, carry):
                    edge = buf[3 if low else nx + 2, 3 + k, rows, :]
                    slope = edge - buf[4 if low else nx + 1, 3 + k, rows, :]
                    for r in range(1, 4):
                        buf[3 - r if low else nx + 2 + r, 3 + k, rows, :] = edge + r * slope
                    return carry
                lax.fori_loop(0, nh, body, 0)
            return act
        pl.when(gx == 0)(ends(True))
        pl.when(gx == ngx - 1)(ends(False))

    def fill_y(buf, t):
        index = lax.broadcasted_iota(jnp.int32, (8, nv), 0).astype(jnp.float32)

        def ends(low):
            reach = (8.0 - index) if low else (index + 1.0)
            at, near, to = (PAD, PAD + 1, 0) if low else (PAD + ny - 1, PAD + ny - 2, PAD + ny)

            def act():
                def body(x, carry):
                    for k in range(nh):
                        edge = buf[3 + x, 3 + k, at:at + 1, :]
                        slope = edge - buf[3 + x, 3 + k, near:near + 1, :]
                        buf[3 + x, 3 + k, to:to + 8, :] = edge + reach * slope
                    return carry
                lax.fori_loop(0, nx, body, 0)
            return act
        if t == 0:
            pl.when(gy == 0)(ends(True))
        if t == tiles - 1:
            pl.when(gy == ngy - 1)(ends(False))

    def open_x(t, far):
        for c in range(len(heads)):
            if far and c in RELAYED:
                continue
            for way, (copy, _, _) in enumerate(plans[0]["x", t, c]):
                under(gx == 1 + way if far else lax.rem(gx, 2) == way, copy.start)
            if c in RELAYED:
                for out, _, from_here, _ in legs(0, t, c):
                    under(from_here, out.start)

    def open_h(t, far):
        for p in range(len(planes)):
            for way, (copy, _, _) in enumerate(plans[0]["h", t, p]):
                edge = (nha - 1) * (1 - way)
                under(ha == edge if far else ha != edge, copy.start)

    def open_y(t):
        for c in range(len(planes)):
            send(0, "y", t, c)

    def open_tile(t, along_x=True, along_h=True):
        if bending and along_x:
            open_x(t, False)
            open_x(t, True)
        if bending and along_h:
            open_h(t, False)
            open_h(t, True)

    if bending:
        open_h(0, False)
        open_x(0, False)
        open_y(tiles - 1)
        signal(far_x, {"gx": beside})()
        under(ha == 1, signal(low_in, {"ha": ha + 1}))
        under(ha == nha - 2, signal(high_in, {"ha": ha - 1}))
        open_y(0) if tiles > 1 else None

        @pl.when((ha > 1) & (ha < nha - 1))
        def _():
            await_one(low_in)()
            signal(low_in, {"ha": ha + 1})()

        @pl.when((ha > 0) & (ha < nha - 2))
        def _():
            await_one(high_in)()
            signal(high_in, {"ha": ha - 1})()

        await_one(far_x)()
        open_x(0, True)
        for copy in rate_copies:
            copy.start()
        v_pass(b0, 0)
        under(ha == nha - 1, await_one(low_in))
        under(ha == 0, await_one(high_in))
        open_h(0, True)
    else:
        for t in range(tiles):
            for p in range(len(planes)):
                send(0, "h", t, p)
                send(0, "y", t, p)
            for way in range(2):
                send_x(0, t, way)
        for copy in rate_copies:
            copy.start()
        v_pass(b0, 0)
    for s in range(3):
        fill_y(bufs[s], 0)
        fill_y(bufs[s], tiles - 1) if tiles > 1 else None
        for t in range(1, tiles):
            yv_pass(s, t - 1)
            if s == 0:
                forward(s, t - 1)
                open_tile(t)
        y_pass(s, tiles - 1)
        forward(s, tiles - 1)
        for t in range(tiles):
            fill_x(bufs[s], t)
            x_pass(s, t)
            if s == 0 and t == 0:
                settle_rate()
            if s < 2 and t > 0:
                forward(s + 1, t - 1)
            h_pass(s, t)
            if s < 2 and t == 0:
                v_pass(bufs[s + 1], 0)

    for copy in rate_copies:
        copy.wait_send()
    for s in range(3):
        for row in plans[s].values():
            for copy, has_out, _ in row:
                under(has_out, copy.wait_send)
        if bending:
            for t in range(tiles):
                for c in RELAYED:
                    for out, on, from_here, here in legs(s, t, c):
                        under(from_here, out.wait_send)
                        under(here, on.wait_send)


def tables(nv, n_head):
    speeds = (SPEED_LOW + SPEED_SPAN * (np.arange(nv, dtype=np.float32) + np.float32(0.5)) / nv).astype(np.float32)
    angles = np.arange(n_head, dtype=np.float32) * np.float32(2.0 * math.pi / n_head)
    turns = np.stack([np.cos(angles.astype(np.float64)), np.sin(angles.astype(np.float64))])
    flow = (turns[:, :, None] * speeds[None, None, :] / CELL_SIZE).astype(np.float32)
    ends = np.concatenate([flow[:, :, 0], flow[:, :, -1]], axis=1)
    rows = -(-ends.shape[1] // 128)
    ends = np.concatenate([ends, np.repeat(ends[:, :1], rows * 128 - ends.shape[1], axis=1)], axis=1)
    return flow, ends.reshape(2, rows, 128)


def solution(mesh):
    axes = (mesh.shape["gx"], mesh.shape["gy"], mesh.shape["ha"])

    def body(level_set, wind_field):
        nx, ny, nh, nv = level_set.shape
        flow, ends = tables(nv, nh * axes[2])
        n_xy = axes[0] * axes[1]
        tiles = ny // 8
        count = n_copies(nx, nh, tiles)
        state = pltpu.VMEM((nx + 6, nh + 6, ny + 2 * PAD, nv), jnp.float32)
        cells = pltpu.VMEM((nx, nh, ny, nv), jnp.float32)
        vmem = pl.BlockSpec(memory_space=pltpu.VMEM)
        increment = pl.pallas_call(
            functools.partial(kernel, (nx, ny, nh, nv), axes),
            out_shape=pltpu.VMEM((nx, nh, ny, nv), jnp.float32),
            in_specs=[pl.BlockSpec(memory_space=pltpu.HBM)] * 4,
            out_specs=vmem,
            scratch_shapes=[
                state, state, state, cells, cells, cells,
                pltpu.SMEM((2, nx, ny), jnp.float32),
                pltpu.VMEM(flow.shape, jnp.float32),
                pltpu.VMEM(ends.shape, jnp.float32),
                pltpu.VMEM((2, 2, nh // 2, 8, nv), jnp.float32),
                pltpu.VMEM((2, 7, nh // 2, 8, nv), jnp.float32),
                pltpu.VMEM((2, nx, ny, nv), jnp.float32),
                pltpu.VMEM((8, 128), jnp.float32),
                pltpu.VMEM((n_xy - 1, 8, 128), jnp.float32),
                pltpu.VMEM((8, nv), jnp.float32),
                pltpu.VMEM((3, 3, nh, ny, nv), jnp.float32),
                pltpu.SemaphoreType.DMA((3, count)),
                pltpu.SemaphoreType.DMA((3, count)),
                pltpu.SemaphoreType.DMA((n_xy - 1,)),
                pltpu.SemaphoreType.DMA((n_xy - 1,)),
                pltpu.SemaphoreType.DMA((4,)),
                pltpu.SemaphoreType.DMA((3, tiles, len(RELAYED), 2)),
                pltpu.SemaphoreType.DMA((3, tiles, len(RELAYED), 2)),
                pltpu.SemaphoreType.REGULAR,
                pltpu.SemaphoreType.REGULAR,
                pltpu.SemaphoreType.REGULAR,
            ],
            compiler_params=pltpu.CompilerParams(
                collective_id=0, has_side_effects=True, vmem_limit_bytes=56 * 2**20
            ),
        )(level_set.transpose(0, 2, 1, 3), wind_field, jnp.asarray(flow), jnp.asarray(ends))
        return increment.transpose(0, 2, 1, 3)

    return jax.shard_map(
        body,
        mesh=mesh,
        in_specs=(P("gx", "gy", "ha", None), P(None, "gx", "gy")),
        out_specs=P("gx", "gy", "ha", None),
        check_vma=False,
    )
```

```python
import functools
import math

import jax
import jax.numpy as jnp
import numpy as np
from jax import lax
from jax.experimental import pallas as pl
from jax.experimental.pallas import tpu as pltpu
from jax.sharding import PartitionSpec as P

CELL_SIZE = 0.05
SPEED_LOW = 0.1
SPEED_SPAN = 0.4
TURN_MAX = 1.0
ACCEL_MAX = 0.05
CFL_NUMBER = 0.5
WENO_EPS = 1e-06
SCALE = 32.0
PAD = 8
MESH = pl.DeviceIdType.MESH


def rcp(d):
    return pl.reciprocal(d, approx=False)


def eps_of(spacing):
    return 0.75 * WENO_EPS * (spacing * SCALE) ** 2


def smooth(d2, d3, e1, e2, e3, eps):
    g2 = 0.75 * d2
    g3 = 0.75 * d3
    c3 = g3 * d3 + eps
    s1 = e1 * (e1 + g2) + (g2 * d2 + eps)
    s2 = e2 * (e2 - g3) + c3
    s3 = e3 * (e3 - g3) + c3
    return s1, s2, s3


def upwind(dm2, dm1, d0, dp1, dp2, c0, c1, fh, eps):
    pos = fh > 0.0
    d1 = jnp.where(pos, dp2, dm2)
    d2 = jnp.where(pos, dp1, dm1)
    d4 = jnp.where(pos, dm1, dp1)
    c = jnp.where(pos, c1, c0)
    d3 = d0
    e1 = d2 - d1
    e2 = d3 - d2
    e3 = d4 - d3
    s1, s2, s3 = smooth(d2, d3, e1, e2, e3, eps)
    t1 = s2 * s3
    t2 = s1 * s3
    t3 = s1 * s2
    r1 = t1 * t1
    r2 = t2 * t2
    w3 = 1.5 * (t3 * t3)
    num = r1 * (e1 - e2) + w3 * (e2 - e3)
    den = (r1 + 6.0 * r2) + (w3 + w3)
    q = (d3 + 0.5 * d2) + num * rcp(den)
    return q * (jnp.abs(fh) * (1.0 / 3.0)) - c * fh


def triple(da, db, eps):
    e = db - da
    s2 = e * e + (0.75 * (da * db) + eps)
    h = 1.5 * e
    return e, s2 + db * h, s2, s2 - da * h


def face_pair(c, d2, d3, e1, e2, e3, s1, s2, s3):
    t1 = s2 * s3
    t2 = s1 * s3
    t3 = s1 * s2
    r1 = t1 * t1
    r2 = t2 * t2
    r3 = t3 * t3
    a = r1 * (e1 - e2)
    b = r3 * (e2 - e3)
    m = 6.0 * r2 + (r1 + r3)
    n = a + b
    left = (3.0 * c + (d3 + 0.5 * d2)) + (n + 0.5 * b) * rcp(m + (r3 + r3))
    right = ((d2 + 0.5 * d3) - 3.0 * c) + (n + 0.5 * a) * rcp(m + (r1 + r1))
    return left, right


def head_chunks(nh):
    half = nh // 2
    return ((0, half), (half, nh - half))


RELAYED = (1,)


def folded(axes):
    return axes[0] == 4 and axes[1] == 2 and axes[2] > 2


def plane_chunks(nx):
    half = nx // 2
    return ((0, half), (half, nx - half))


def n_copies(nx, nh, tiles):
    return 2 * len(plane_chunks(nx)) * (tiles + 1) + 2 * len(head_chunks(nh)) * tiles


def kernel(sizes, axes, u_hbm, wind_hbm, flow_hbm, rate_hbm, out_ref,
           b0, b1, b2, acc, rights, u_ref, wind_ref, flow_ref, rate_ref, va, vb, wind, best, peers, step, relay,
           sends, recvs, rsend, rrecv, isem, lsend, lrecv, far_x, low_in, high_in):
    nx, ny, nh, nv = sizes
    ngx, ngy, nha = axes
    bufs = (b0, b1, b2)
    d_theta = 2.0 * math.pi / (nh * nha)
    d_speed = SPEED_SPAN / nv
    tiles = ny // 8
    group = nh // 2
    heads, planes = head_chunks(nh), plane_chunks(nx)
    gx, gy, ha = lax.axis_index("gx"), lax.axis_index("gy"), lax.axis_index("ha")
    n_xy = ngx * ngy
    me = gx * ngy + gy

    def peer(delta):
        other = lax.rem(me + delta, n_xy)
        return {"gx": other // ngy, "gy": lax.rem(other, ngy)}

    up_ha = {"ha": lax.rem(ha + 1, nha)}
    down_ha = {"ha": lax.rem(ha + nha - 1, nha)}
    bending = folded(axes)
    beside, across = gx + 1 - 2 * lax.rem(gx, 2), lax.rem(gx + 2, 4)
    near = ({"gy": 1 - gy}, {"gx": beside}, {"gx": across},
            {"gx": beside, "gy": 1 - gy}, {"gx": across, "gy": 1 - gy})

    def under(condition, act):
        if condition is None:
            act()
        else:
            pl.when(condition)(act)

    def signal(semaphore, target):
        return lambda: pl.semaphore_signal(semaphore, inc=1, device_id=target, device_id_type=MESH)

    def await_one(semaphore):
        return lambda: pl.semaphore_wait(semaphore, 1)

    barrier = pltpu.get_barrier_semaphore()
    if bending:
        for target in near:
            signal(barrier, target)()
        under(ha < nha - 1, signal(barrier, {"ha": ha + 1}))
        under(ha > 0, signal(barrier, {"ha": ha - 1}))
    else:
        for delta in range(1, n_xy):
            signal(barrier, peer(delta))()
        for target in (up_ha, down_ha):
            signal(barrier, target)()

    fetches = [
        pltpu.make_async_copy(src, dst, isem.at[i])
        for i, (src, dst) in enumerate((
            (wind_hbm, wind_ref), (rate_hbm, rate_ref), (u_hbm, u_ref), (flow_hbm, flow_ref)))
    ]
    for fetch in fetches:
        fetch.start()
    for fetch in fetches:
        fetch.wait()

    def load_plane(x, carry):
        for k in range(nh):
            b0[3 + x, 3 + k, PAD:PAD + ny, :] = u_ref[x, k] * SCALE
        for comp in range(2):
            for y in range(ny):
                wind[comp, x, y:y + 1, :] = jnp.full((1, nv), wind_ref[comp, x, y] * (1.0 / CELL_SIZE), jnp.float32)
        return carry

    lax.fori_loop(0, nx, load_plane, 0)

    def rate_plane(x, top):
        for r in range(rate_ref.shape[1]):
            for t in range(tiles):
                fx = rate_ref[0, r:r + 1, :] + wind[0, x, 8 * t:8 * t + 8, :]
                fy = rate_ref[1, r:r + 1, :] + wind[1, x, 8 * t:8 * t + 8, :]
                top = jnp.maximum(top, jnp.abs(fx) + jnp.abs(fy))
        return top

    best[...] = lax.fori_loop(0, nx, rate_plane, jnp.zeros((8, 128), jnp.float32))

    if bending:
        beyond = (ha + nha - 2) // (nha - 1) + (2 * nha - 3 - ha) // (nha - 1)
        pl.semaphore_wait(barrier, len(near) + beyond)
    else:
        pl.semaphore_wait(barrier, n_xy + 1)

    def tile_rows(t):
        return pl.ds(PAD + 8 * t, 8)

    places = []

    def copies(s):
        buf = bufs[s]
        plans = {}
        for t in range(tiles):
            ys = tile_rows(t)
            for c, (x0, count) in enumerate(planes):
                xs = pl.ds(3 + x0, count)
                plans["h", t, c] = (
                    (buf.at[xs, pl.ds(nh, 3), ys], buf.at[xs, pl.ds(0, 3), ys], up_ha, None, None),
                    (buf.at[xs, pl.ds(3, 3), ys], buf.at[xs, pl.ds(3 + nh, 3), ys], down_ha, None, None),
                )
            for c, (k0, count) in enumerate(heads):
                hc = pl.ds(3 + k0, count)
                around = bending and c in RELAYED
                plans["x", t, c] = (
                    (buf.at[pl.ds(nx, 3), hc, ys], buf.at[pl.ds(0, 3), hc, ys], {"gx": gx + 1},
                     (gx == 0) | (gx == 2) if around else gx < ngx - 1, gx > 0),
                    (buf.at[pl.ds(3, 3), hc, ys], buf.at[pl.ds(3 + nx, 3), hc, ys], {"gx": gx - 1},
                     (gx == 1) | (gx == 3) if around else gx > 0, gx < ngx - 1),
                )
        hc = pl.ds(3, nh)
        for c, (x0, count) in enumerate(planes):
            xs = pl.ds(3 + x0, count)
            plans["y", tiles - 1, c] = (
                (buf.at[xs, hc, pl.ds(ny, PAD)], buf.at[xs, hc, pl.ds(0, PAD)], {"gy": gy + 1},
                 gy < ngy - 1, gy > 0),
            )
            plans["y", 0, c] = plans.get(("y", 0, c), ()) + (
                (buf.at[xs, hc, pl.ds(PAD, PAD)], buf.at[xs, hc, pl.ds(PAD + ny, PAD)], {"gy": gy - 1},
                 gy > 0, gy < ngy - 1),
            )
        made, at, starts = {}, 0, {}
        for key, group_of in plans.items():
            row = []
            starts[key] = at
            for src, dst, target, has_out, has_in in group_of:
                row.append((pltpu.make_async_remote_copy(
                    src_ref=src, dst_ref=dst, send_sem=sends.at[s, at], recv_sem=recvs.at[s, at],
                    device_id=target, device_id_type=MESH), has_out, has_in))
                at += 1
            made[key] = row
        places.append(starts)
        return made

    rate_copies = [
        pltpu.make_async_remote_copy(
            src_ref=best, dst_ref=peers.at[delta - 1], send_sem=rsend.at[delta - 1],
            recv_sem=rrecv.at[delta - 1], device_id=peer(delta), device_id_type=MESH)
        for delta in range(1, n_xy)
    ]

    def settle_rate():
        top = best[...]
        for i, copy in enumerate(rate_copies):
            copy.wait_recv()
            top = jnp.maximum(top, peers[i])
        rate = jnp.max(top, axis=(0, 1), keepdims=True) + (TURN_MAX / d_theta + ACCEL_MAX / d_speed)
        step[...] = jnp.broadcast_to(CFL_NUMBER / rate, step.shape)

    plans = [copies(s) for s in range(3)]

    built = {}

    def legs(s, t, c):
        if (s, t, c) in built:
            return built[s, t, c]
        buf = bufs[s]
        k0, count = heads[c]
        hc, ys = pl.ds(3 + k0, count), tile_rows(t)
        held = relay.at[s, pl.ds(0, 3), pl.ds(k0, count), pl.ds(8 * t, 8)]
        i = RELAYED.index(c)
        rows = []
        for way, (src, dst, origin, middle, end) in enumerate((
            (buf.at[pl.ds(nx, 3), hc, ys], buf.at[pl.ds(0, 3), hc, ys], 1, 3, 2),
            (buf.at[pl.ds(3, 3), hc, ys], buf.at[pl.ds(3 + nx, 3), hc, ys], 2, 0, 1),
        )):
            out = pltpu.make_async_remote_copy(
                src_ref=src, dst_ref=held, send_sem=lsend.at[s, t, i, way], recv_sem=lrecv.at[s, t, i, way],
                device_id={"gx": middle}, device_id_type=MESH)
            on = pltpu.make_async_remote_copy(
                src_ref=held, dst_ref=dst, send_sem=sends.at[s, places[s]["x", t, c] + way],
                recv_sem=recvs.at[s, places[s]["x", t, c] + way],
                device_id={"gx": end}, device_id_type=MESH)
            rows.append((out, on, gx == origin, gx == middle))
        built[s, t, c] = rows
        return rows

    def forward(s, t):
        if bending:
            for c in RELAYED:
                for out, on, _, here in legs(s, t, c):
                    @pl.when(here)
                    def _():
                        out.wait_recv()
                        on.start()

    def send(s, *key):
        for copy, has_out, _ in plans[s].get(key, ()):
            under(has_out, copy.start)

    def send_x(s, t, way):
        for c in range(len(heads)):
            copy, has_out, _ = plans[s]["x", t, c][way]
            under(has_out, copy.start)
            if bending and c in RELAYED:
                out, _, from_here, _ = legs(s, t, c)[way]
                under(from_here, out.start)

    def wait_in(s, *key):
        for copy, _, has_in in plans[s].get(key, ()):
            under(has_in, copy.wait_recv)

    def v_parts(buf, t):
        eps = eps_of(d_speed)
        coef = ACCEL_MAX / (3.0 * d_speed)
        e4 = np.float32(np.float32(eps * eps) ** 2)
        lane = lax.broadcasted_iota(jnp.int32, (8, nv), 1)
        edge = lane == 0
        keep = jnp.where((lane == 0) | (lane == nv - 1), 0.0, 1.0)
        inner_lane = jnp.where(edge, 0.0, 1.0)
        rows, rows_acc = tile_rows(t), slice(8 * t, 8 * t + 8)

        def first(x, half):
            for j in range(group):
                u = buf[3 + x, 3 + half * group + j, rows, :]
                q = u - pltpu.roll(u, 1, 1)
                va[half, 0, j] = q
                va[half, 1, j] = ((pltpu.roll(u, nv - 1, 1) - u) - q) * keep

        def second(half):
            for j in range(group):
                q, d = va[half, 0, j], va[half, 1, j]
                vb[half, 0, j] = pltpu.roll(d, 2, 1)
                vb[half, 1, j] = pltpu.roll(d, 1, 1)
                vb[half, 2, j] = d
                vb[half, 3, j] = pltpu.roll(d, nv - 1, 1)
                vb[half, 4, j] = pltpu.roll(q, 1, 1)
                vb[half, 5, j] = q
                vb[half, 6, j] = pltpu.roll(q, nv - 1, 1)

        def third(x, half):
            for j in range(group):
                k = half * group + j
                d1, d2, d3, d4, qb, qc, qd = [vb[half, i, j] for i in range(7)]
                e1 = d2 - d1
                e2 = d3 - d2
                e3 = d4 - d3
                s1, s2, s3 = smooth(d2, d3, e1, e2, e3, eps)
                t1 = s2 * s3
                t2 = s1 * s3
                t3 = s1 * s2
                r1 = t1 * t1
                r2 = t2 * t2
                r3 = t3 * t3
                f12 = e1 - e2
                f23 = e2 - e3
                r2l = jnp.where(edge, r1, r2)
                r3l = jnp.where(edge, e4, r3)
                r2r = jnp.where(edge, r3, r2)
                r1r = jnp.where(edge, e4, r1)
                cl = jnp.where(edge, qd, qc)
                cr = jnp.where(edge, qb, qc)
                nl = r1 * (f12 * inner_lane) + 1.5 * (r3l * f23)
                nr = 1.5 * (r1r * f12) + r3 * (f23 * inner_lane)
                left = (3.0 * cl + (d3 + 0.5 * d2)) + nl * rcp(r1 + 6.0 * r2l + 3.0 * r3l)
                right = ((d2 + 0.5 * d3) - 3.0 * cr) + nr * rcp(3.0 * r1r + 6.0 * r2r + r3)
                acc[x, k, rows_acc, :] = coef * left
                rights[x, k, rows_acc, :] = coef * right

        def begin():
            first(0, 0)
            first(0, 1)
            second(0)

        def body(x, carry):
            after = jnp.minimum(x + 1, nx - 1)
            third(x, 0)
            second(1)
            first(after, 0)
            third(x, 1)
            second(0)
            first(after, 1)
            return carry

        return begin, body

    def v_pass(buf, t):
        begin, body = v_parts(buf, t)
        begin()
        lax.fori_loop(0, nx, body, 0)

    def h_pass(s, t):
        buf = bufs[s]
        eps = eps_of(d_theta)
        coef = TURN_MAX / (3.0 * d_theta)
        rows, rows_acc = tile_rows(t), pl.ds(8 * t, 8)

        def body(x, carry):
            dt = step[...]
            u = [buf[3 + x, j, rows, :] for j in range(nh + 6)]
            q = [u[j + 1] - u[j] for j in range(nh + 5)]
            d = [q[j + 1] - q[j] for j in range(nh + 4)]
            tr = [triple(d[j], d[j + 1], eps) for j in range(nh + 3)]
            before = None
            for f in range(nh + 1):
                left, right = face_pair(
                    q[f + 2], d[f + 1], d[f + 2], tr[f][0], tr[f + 1][0], tr[f + 2][0],
                    tr[f][1], tr[f + 1][2], tr[f + 2][3])
                if before is not None:
                    k = f - 1
                    total = acc[x, k, rows_acc, :] + coef * jnp.minimum(before, right)
                    moved = u[k + 3] - dt * jnp.maximum(total, 0.0)
                    if s == 0:
                        b1[3 + x, 3 + k, rows, :] = moved
                    elif s == 1:
                        b2[3 + x, 3 + k, rows, :] = 0.75 * b0[3 + x, 3 + k, rows, :] + 0.25 * moved
                    else:
                        out_ref[x, k, rows_acc, :] = (moved - b0[3 + x, 3 + k, rows, :]) * (2.0 / (3.0 * SCALE))
                before = left
            return carry

        for c, (x0, count) in enumerate(planes):
            wait_in(s, "h", t, c)
            lax.fori_loop(x0, x0 + count, body, 0)
            if s < 2:
                send(s + 1, "h", t, c)
                if c == 0:
                    send_x(s + 1, t, 1)
                if c == len(planes) - 1:
                    send_x(s + 1, t, 0)
                send(s + 1, "y", t, c)

    def flow_row(comp, k):
        return flow_ref[comp, pl.ds(ha * nh + k, 1), :]

    def y_parts(s, t):
        buf = bufs[s]
        eps = eps_of(CELL_SIZE)
        rows = slice(8 * t, 8 * t + 8)

        def begin():
            for c in range(len(planes)):
                if t == 0:
                    for copy, _, has_in in plans[s]["y", tiles - 1, c][:1]:
                        under(has_in, copy.wait_recv)
                if t == tiles - 1:
                    for copy, _, has_in in plans[s]["y", 0, c][-1:]:
                        under(has_in, copy.wait_recv)

        def body(x, carry):
            for k in range(nh):
                u = [buf[3 + x, 3 + k, PAD + 8 * t + j:PAD + 8 * t + j + 8, :] for j in range(-3, 4)]
                q = [u[j + 1] - u[j] for j in range(6)]
                d = [q[j + 1] - q[j] for j in range(5)]
                fh = flow_row(1, k) + wind[1, x, rows, :]
                along_v = jnp.minimum(acc[x, k, rows, :], pltpu.roll(rights[x, k, rows, :], nv - 1, 1))
                acc[x, k, rows, :] = along_v + upwind(*d, q[2], q[3], fh, eps)
            return carry

        return begin, body

    def y_pass(s, t):
        begin, body = y_parts(s, t)
        begin()
        lax.fori_loop(0, nx, body, 0)

    def yv_pass(s, t):
        y_begin, y_body = y_parts(s, t)
        v_begin, v_body = v_parts(bufs[s], t + 1)
        v_begin()
        y_begin()

        def body(x, carry):
            y_body(x, carry)
            v_body(x, carry)
            return carry

        lax.fori_loop(0, nx, body, 0)

    def x_pass(s, t):
        buf = bufs[s]
        eps = eps_of(CELL_SIZE)
        rows, rows_acc = tile_rows(t), pl.ds(8 * t, 8)

        def body(k, carry):
            row = flow_row(0, k)
            u = [buf[j, 3 + k, rows, :] for j in range(nx + 6)]
            q = [u[j + 1] - u[j] for j in range(nx + 5)]
            d = [q[j + 1] - q[j] for j in range(nx + 4)]
            for x in range(nx):
                fh = row + wind[0, x, rows_acc, :]
                acc[x, k, rows_acc, :] += upwind(*d[x:x + 5], q[x + 2], q[x + 3], fh, eps)
            return carry

        for c, (k0, count) in enumerate(heads):
            wait_in(s, "x", t, c)
            lax.fori_loop(k0, k0 + count, body, 0)

    def fill_x(buf, t):
        rows = tile_rows(t)

        def ends(low):
            def act():
                def body(k, carry):
                    edge = buf[3 if low else nx + 2, 3 + k, rows, :]
                    slope = edge - buf[4 if low else nx + 1, 3 + k, rows, :]
                    for r in range(1, 4):
                        buf[3 - r if low else nx + 2 + r, 3 + k, rows, :] = edge + r * slope
                    return carry
                lax.fori_loop(0, nh, body, 0)
            return act
        pl.when(gx == 0)(ends(True))
        pl.when(gx == ngx - 1)(ends(False))

    def fill_y(buf, t):
        index = lax.broadcasted_iota(jnp.int32, (8, nv), 0).astype(jnp.float32)

        def ends(low):
            reach = (8.0 - index) if low else (index + 1.0)
            at, near, to = (PAD, PAD + 1, 0) if low else (PAD + ny - 1, PAD + ny - 2, PAD + ny)

            def act():
                def body(x, carry):
                    for k in range(nh):
                        edge = buf[3 + x, 3 + k, at:at + 1, :]
                        slope = edge - buf[3 + x, 3 + k, near:near + 1, :]
                        buf[3 + x, 3 + k, to:to + 8, :] = edge + reach * slope
                    return carry
                lax.fori_loop(0, nx, body, 0)
            return act
        if t == 0:
            pl.when(gy == 0)(ends(True))
        if t == tiles - 1:
            pl.when(gy == ngy - 1)(ends(False))

    def open_x(t, far):
        for c in range(len(heads)):
            if far and c in RELAYED:
                continue
            for way, (copy, _, _) in enumerate(plans[0]["x", t, c]):
                under(gx == 1 + way if far else lax.rem(gx, 2) == way, copy.start)
            if c in RELAYED:
                for out, _, from_here, _ in legs(0, t, c):
                    under(from_here, out.start)

    def open_h(t, far):
        for p in range(len(planes)):
            for way, (copy, _, _) in enumerate(plans[0]["h", t, p]):
                edge = (nha - 1) * (1 - way)
                under(ha == edge if far else ha != edge, copy.start)

    def open_y(t):
        for c in range(len(planes)):
            send(0, "y", t, c)

    def open_tile(t, along_x=True, along_h=True):
        if bending and along_x:
            open_x(t, False)
            open_x(t, True)
        if bending and along_h:
            for p in range(1, len(planes)):
                for way, (copy, _, _) in enumerate(plans[0]["h", t, p]):
                    under(ha != (nha - 1) * (1 - way), copy.start)
            open_h(t, True)

    if bending:
        open_h(0, False)
        open_x(0, False)
        open_y(tiles - 1)
        signal(far_x, {"gx": beside})()
        under(ha == 1, signal(low_in, {"ha": ha + 1}))
        under(ha == nha - 2, signal(high_in, {"ha": ha - 1}))
        open_y(0) if tiles > 1 else None

        @pl.when((ha > 1) & (ha < nha - 1))
        def _():
            await_one(low_in)()
            signal(low_in, {"ha": ha + 1})()

        @pl.when((ha > 0) & (ha < nha - 2))
        def _():
            await_one(high_in)()
            signal(high_in, {"ha": ha - 1})()

        await_one(far_x)()
        open_x(0, True)
        for t in range(1, tiles):
            for way, (copy, _, _) in enumerate(plans[0]["h", t, 0]):
                under(ha != (nha - 1) * (1 - way), copy.start)
        for copy in rate_copies:
            copy.start()
        v_pass(b0, 0)
        under(ha == nha - 1, await_one(low_in))
        under(ha == 0, await_one(high_in))
        open_h(0, True)
    else:
        for t in range(tiles):
            for p in range(len(planes)):
                send(0, "h", t, p)
                send(0, "y", t, p)
            for way in range(2):
                send_x(0, t, way)
        for copy in rate_copies:
            copy.start()
        v_pass(b0, 0)
    for s in range(3):
        fill_y(bufs[s], 0)
        fill_y(bufs[s], tiles - 1) if tiles > 1 else None
        for t in range(1, tiles):
            yv_pass(s, t - 1)
            if s == 0:
                forward(s, t - 1)
                open_tile(t)
        y_pass(s, tiles - 1)
        if tiles == 1:
            forward(s, 0)
        for t in range(tiles):
            fill_x(bufs[s], t)
            x_pass(s, t)
            if t == 0 and tiles > 1:
                forward(s, tiles - 1)
            if s == 0 and t == 0:
                settle_rate()
            if s < 2 and t > 0:
                forward(s + 1, t - 1)
            h_pass(s, t)
            if s < 2 and t == 0:
                v_pass(bufs[s + 1], 0)

    for copy in rate_copies:
        copy.wait_send()
    for s in range(3):
        for row in plans[s].values():
            for copy, has_out, _ in row:
                under(has_out, copy.wait_send)
        if bending:
            for t in range(tiles):
                for c in RELAYED:
                    for out, on, from_here, here in legs(s, t, c):
                        under(from_here, out.wait_send)
                        under(here, on.wait_send)


def tables(nv, n_head):
    speeds = (SPEED_LOW + SPEED_SPAN * (np.arange(nv, dtype=np.float32) + np.float32(0.5)) / nv).astype(np.float32)
    angles = np.arange(n_head, dtype=np.float32) * np.float32(2.0 * math.pi / n_head)
    turns = np.stack([np.cos(angles.astype(np.float64)), np.sin(angles.astype(np.float64))])
    flow = (turns[:, :, None] * speeds[None, None, :] / CELL_SIZE).astype(np.float32)
    ends = np.concatenate([flow[:, :, 0], flow[:, :, -1]], axis=1)
    rows = -(-ends.shape[1] // 128)
    ends = np.concatenate([ends, np.repeat(ends[:, :1], rows * 128 - ends.shape[1], axis=1)], axis=1)
    return flow, ends.reshape(2, rows, 128)


def solution(mesh):
    axes = (mesh.shape["gx"], mesh.shape["gy"], mesh.shape["ha"])

    def body(level_set, wind_field):
        nx, ny, nh, nv = level_set.shape
        flow, ends = tables(nv, nh * axes[2])
        n_xy = axes[0] * axes[1]
        tiles = ny // 8
        count = n_copies(nx, nh, tiles)
        state = pltpu.VMEM((nx + 6, nh + 6, ny + 2 * PAD, nv), jnp.float32)
        cells = pltpu.VMEM((nx, nh, ny, nv), jnp.float32)
        vmem = pl.BlockSpec(memory_space=pltpu.VMEM)
        increment = pl.pallas_call(
            functools.partial(kernel, (nx, ny, nh, nv), axes),
            out_shape=pltpu.VMEM((nx, nh, ny, nv), jnp.float32),
            in_specs=[pl.BlockSpec(memory_space=pltpu.HBM)] * 4,
            out_specs=vmem,
            scratch_shapes=[
                state, state, state, cells, cells, cells,
                pltpu.SMEM((2, nx, ny), jnp.float32),
                pltpu.VMEM(flow.shape, jnp.float32),
                pltpu.VMEM(ends.shape, jnp.float32),
                pltpu.VMEM((2, 2, nh // 2, 8, nv), jnp.float32),
                pltpu.VMEM((2, 7, nh // 2, 8, nv), jnp.float32),
                pltpu.VMEM((2, nx, ny, nv), jnp.float32),
                pltpu.VMEM((8, 128), jnp.float32),
                pltpu.VMEM((n_xy - 1, 8, 128), jnp.float32),
                pltpu.VMEM((8, nv), jnp.float32),
                pltpu.VMEM((3, 3, nh, ny, nv), jnp.float32),
                pltpu.SemaphoreType.DMA((3, count)),
                pltpu.SemaphoreType.DMA((3, count)),
                pltpu.SemaphoreType.DMA((n_xy - 1,)),
                pltpu.SemaphoreType.DMA((n_xy - 1,)),
                pltpu.SemaphoreType.DMA((4,)),
                pltpu.SemaphoreType.DMA((3, tiles, len(RELAYED), 2)),
                pltpu.SemaphoreType.DMA((3, tiles, len(RELAYED), 2)),
                pltpu.SemaphoreType.REGULAR,
                pltpu.SemaphoreType.REGULAR,
                pltpu.SemaphoreType.REGULAR,
            ],
            compiler_params=pltpu.CompilerParams(
                collective_id=0, has_side_effects=True, vmem_limit_bytes=56 * 2**20
            ),
        )(level_set.transpose(0, 2, 1, 3), wind_field, jnp.asarray(flow), jnp.asarray(ends))
        return increment.transpose(0, 2, 1, 3)

    return jax.shard_map(
        body,
        mesh=mesh,
        in_specs=(P("gx", "gy", "ha", None), P(None, "gx", "gy")),
        out_specs=P("gx", "gy", "ha", None),
        check_vma=False,
    )
```

```python
import functools
import math

import jax
import jax.numpy as jnp
import numpy as np
from jax import lax
from jax.experimental import pallas as pl
from jax.experimental.pallas import tpu as pltpu
from jax.sharding import PartitionSpec as P

CELL_SIZE = 0.05
SPEED_LOW = 0.1
SPEED_SPAN = 0.4
TURN_MAX = 1.0
ACCEL_MAX = 0.05
CFL_NUMBER = 0.5
WENO_EPS = 1e-06
SCALE = 32.0
PAD = 8
MESH = pl.DeviceIdType.MESH


def rcp(d):
    return pl.reciprocal(d, approx=False)


def eps_of(spacing):
    return 0.75 * WENO_EPS * (spacing * SCALE) ** 2


def smooth(d2, d3, e1, e2, e3, eps):
    g2 = 0.75 * d2
    g3 = 0.75 * d3
    c3 = g3 * d3 + eps
    s1 = e1 * (e1 + g2) + (g2 * d2 + eps)
    s2 = e2 * (e2 - g3) + c3
    s3 = e3 * (e3 - g3) + c3
    return s1, s2, s3


def upwind(dm2, dm1, d0, dp1, dp2, c0, c1, fh, eps):
    pos = fh > 0.0
    d1 = jnp.where(pos, dp2, dm2)
    d2 = jnp.where(pos, dp1, dm1)
    d4 = jnp.where(pos, dm1, dp1)
    c = jnp.where(pos, c1, c0)
    d3 = d0
    e1 = d2 - d1
    e2 = d3 - d2
    e3 = d4 - d3
    s1, s2, s3 = smooth(d2, d3, e1, e2, e3, eps)
    t1 = s2 * s3
    t2 = s1 * s3
    t3 = s1 * s2
    r1 = t1 * t1
    r2 = t2 * t2
    w3 = 1.5 * (t3 * t3)
    num = r1 * (e1 - e2) + w3 * (e2 - e3)
    den = (r1 + 6.0 * r2) + (w3 + w3)
    q = (d3 + 0.5 * d2) + num * rcp(den)
    return q * (jnp.abs(fh) * (1.0 / 3.0)) - c * fh


def triple(da, db, eps):
    e = db - da
    s2 = e * e + (0.75 * (da * db) + eps)
    h = 1.5 * e
    return e, s2 + db * h, s2, s2 - da * h


def face_pair(c, d2, d3, e1, e2, e3, s1, s2, s3):
    t1 = s2 * s3
    t2 = s1 * s3
    t3 = s1 * s2
    r1 = t1 * t1
    r2 = t2 * t2
    r3 = t3 * t3
    a = r1 * (e1 - e2)
    b = r3 * (e2 - e3)
    m = 6.0 * r2 + (r1 + r3)
    n = a + b
    left = (3.0 * c + (d3 + 0.5 * d2)) + (n + 0.5 * b) * rcp(m + (r3 + r3))
    right = ((d2 + 0.5 * d3) - 3.0 * c) + (n + 0.5 * a) * rcp(m + (r1 + r1))
    return left, right


def head_chunks(nh):
    half = nh // 2
    return ((0, half), (half, nh - half))


RELAYED = (1,)


def folded(axes):
    return axes[0] == 4 and axes[1] == 2 and axes[2] > 2


def plane_chunks(nx):
    half = nx // 2
    return ((0, half), (half, nx - half))


def n_copies(nx, nh, tiles):
    return 2 * len(plane_chunks(nx)) * (tiles + 1) + 2 * len(head_chunks(nh)) * tiles


def kernel(sizes, axes, u_hbm, wind_hbm, flow_hbm, rate_hbm, out_ref,
           b0, b1, b2, acc, rights, u_ref, wind_ref, flow_ref, rate_ref, va, vb, wind, best, peers, step, relay,
           sends, recvs, rsend, rrecv, isem, lsend, lrecv, far_x, low_in, high_in):
    nx, ny, nh, nv = sizes
    ngx, ngy, nha = axes
    bufs = (b0, b1, b2)
    d_theta = 2.0 * math.pi / (nh * nha)
    d_speed = SPEED_SPAN / nv
    tiles = ny // 8
    group = nh // 2
    heads, planes = head_chunks(nh), plane_chunks(nx)
    gx, gy, ha = lax.axis_index("gx"), lax.axis_index("gy"), lax.axis_index("ha")
    n_xy = ngx * ngy
    me = gx * ngy + gy

    def peer(delta):
        other = lax.rem(me + delta, n_xy)
        return {"gx": other // ngy, "gy": lax.rem(other, ngy)}

    up_ha = {"ha": lax.rem(ha + 1, nha)}
    down_ha = {"ha": lax.rem(ha + nha - 1, nha)}
    bending = folded(axes)
    beside, across = gx + 1 - 2 * lax.rem(gx, 2), lax.rem(gx + 2, 4)
    near = ({"gy": 1 - gy}, {"gx": beside}, {"gx": across},
            {"gx": beside, "gy": 1 - gy}, {"gx": across, "gy": 1 - gy})

    def under(condition, act):
        if condition is None:
            act()
        else:
            pl.when(condition)(act)

    def signal(semaphore, target):
        return lambda: pl.semaphore_signal(semaphore, inc=1, device_id=target, device_id_type=MESH)

    def await_one(semaphore):
        return lambda: pl.semaphore_wait(semaphore, 1)

    barrier = pltpu.get_barrier_semaphore()
    if bending:
        for target in near:
            signal(barrier, target)()
        under(ha < nha - 1, signal(barrier, {"ha": ha + 1}))
        under(ha > 0, signal(barrier, {"ha": ha - 1}))
    else:
        for delta in range(1, n_xy):
            signal(barrier, peer(delta))()
        for target in (up_ha, down_ha):
            signal(barrier, target)()

    fetches = [
        pltpu.make_async_copy(src, dst, isem.at[i])
        for i, (src, dst) in enumerate((
            (wind_hbm, wind_ref), (rate_hbm, rate_ref), (u_hbm, u_ref), (flow_hbm, flow_ref)))
    ]
    for fetch in fetches:
        fetch.start()
    for fetch in fetches:
        fetch.wait()

    def load_plane(x, carry):
        for k in range(nh):
            b0[3 + x, 3 + k, PAD:PAD + ny, :] = u_ref[x, k] * SCALE
        for comp in range(2):
            for y in range(ny):
                wind[comp, x, y:y + 1, :] = jnp.full((1, nv), wind_ref[comp, x, y] * (1.0 / CELL_SIZE), jnp.float32)
        return carry

    lax.fori_loop(0, nx, load_plane, 0)

    def rate_plane(x, top):
        for r in range(rate_ref.shape[1]):
            for t in range(tiles):
                fx = rate_ref[0, r:r + 1, :] + wind[0, x, 8 * t:8 * t + 8, :]
                fy = rate_ref[1, r:r + 1, :] + wind[1, x, 8 * t:8 * t + 8, :]
                top = jnp.maximum(top, jnp.abs(fx) + jnp.abs(fy))
        return top

    best[...] = lax.fori_loop(0, nx, rate_plane, jnp.zeros((8, 128), jnp.float32))

    if bending:
        beyond = (ha + nha - 2) // (nha - 1) + (2 * nha - 3 - ha) // (nha - 1)
        pl.semaphore_wait(barrier, len(near) + beyond)
    else:
        pl.semaphore_wait(barrier, n_xy + 1)

    def tile_rows(t):
        return pl.ds(PAD + 8 * t, 8)

    places = []

    def copies(s):
        buf = bufs[s]
        plans = {}
        for t in range(tiles):
            ys = tile_rows(t)
            for c, (x0, count) in enumerate(planes):
                xs = pl.ds(3 + x0, count)
                plans["h", t, c] = (
                    (buf.at[xs, pl.ds(nh, 3), ys], buf.at[xs, pl.ds(0, 3), ys], up_ha, None, None),
                    (buf.at[xs, pl.ds(3, 3), ys], buf.at[xs, pl.ds(3 + nh, 3), ys], down_ha, None, None),
                )
            for c, (k0, count) in enumerate(heads):
                hc = pl.ds(3 + k0, count)
                around = bending and c in RELAYED
                plans["x", t, c] = (
                    (buf.at[pl.ds(nx, 3), hc, ys], buf.at[pl.ds(0, 3), hc, ys], {"gx": gx + 1},
                     (gx == 0) | (gx == 2) if around else gx < ngx - 1, gx > 0),
                    (buf.at[pl.ds(3, 3), hc, ys], buf.at[pl.ds(3 + nx, 3), hc, ys], {"gx": gx - 1},
                     (gx == 1) | (gx == 3) if around else gx > 0, gx < ngx - 1),
                )
        hc = pl.ds(3, nh)
        for c, (x0, count) in enumerate(planes):
            xs = pl.ds(3 + x0, count)
            plans["y", tiles - 1, c] = (
                (buf.at[xs, hc, pl.ds(ny, PAD)], buf.at[xs, hc, pl.ds(0, PAD)], {"gy": gy + 1},
                 gy < ngy - 1, gy > 0),
            )
            plans["y", 0, c] = plans.get(("y", 0, c), ()) + (
                (buf.at[xs, hc, pl.ds(PAD, PAD)], buf.at[xs, hc, pl.ds(PAD + ny, PAD)], {"gy": gy - 1},
                 gy > 0, gy < ngy - 1),
            )
        made, at, starts = {}, 0, {}
        for key, group_of in plans.items():
            row = []
            starts[key] = at
            for src, dst, target, has_out, has_in in group_of:
                row.append((pltpu.make_async_remote_copy(
                    src_ref=src, dst_ref=dst, send_sem=sends.at[s, at], recv_sem=recvs.at[s, at],
                    device_id=target, device_id_type=MESH), has_out, has_in))
                at += 1
            made[key] = row
        places.append(starts)
        return made

    rate_copies = [
        pltpu.make_async_remote_copy(
            src_ref=best, dst_ref=peers.at[delta - 1], send_sem=rsend.at[delta - 1],
            recv_sem=rrecv.at[delta - 1], device_id=peer(delta), device_id_type=MESH)
        for delta in range(1, n_xy)
    ]

    def settle_rate():
        top = best[...]
        for i, copy in enumerate(rate_copies):
            copy.wait_recv()
            top = jnp.maximum(top, peers[i])
        rate = jnp.max(top, axis=(0, 1), keepdims=True) + (TURN_MAX / d_theta + ACCEL_MAX / d_speed)
        step[...] = jnp.broadcast_to(CFL_NUMBER / rate, step.shape)

    plans = [copies(s) for s in range(3)]

    built = {}

    def legs(s, t, c):
        if (s, t, c) in built:
            return built[s, t, c]
        buf = bufs[s]
        k0, count = heads[c]
        hc, ys = pl.ds(3 + k0, count), tile_rows(t)
        held = relay.at[s, pl.ds(0, 3), pl.ds(k0, count), pl.ds(8 * t, 8)]
        i = RELAYED.index(c)
        rows = []
        for way, (src, dst, origin, middle, end) in enumerate((
            (buf.at[pl.ds(nx, 3), hc, ys], buf.at[pl.ds(0, 3), hc, ys], 1, 3, 2),
            (buf.at[pl.ds(3, 3), hc, ys], buf.at[pl.ds(3 + nx, 3), hc, ys], 2, 0, 1),
        )):
            out = pltpu.make_async_remote_copy(
                src_ref=src, dst_ref=held, send_sem=lsend.at[s, t, i, way], recv_sem=lrecv.at[s, t, i, way],
                device_id={"gx": middle}, device_id_type=MESH)
            on = pltpu.make_async_remote_copy(
                src_ref=held, dst_ref=dst, send_sem=sends.at[s, places[s]["x", t, c] + way],
                recv_sem=recvs.at[s, places[s]["x", t, c] + way],
                device_id={"gx": end}, device_id_type=MESH)
            rows.append((out, on, gx == origin, gx == middle))
        built[s, t, c] = rows
        return rows

    def forward(s, t):
        if bending:
            for c in RELAYED:
                for out, on, _, here in legs(s, t, c):
                    @pl.when(here)
                    def _():
                        out.wait_recv()
                        on.start()

    def send(s, *key):
        for copy, has_out, _ in plans[s].get(key, ()):
            under(has_out, copy.start)

    def send_x(s, t, way):
        for c in range(len(heads)):
            copy, has_out, _ = plans[s]["x", t, c][way]
            under(has_out, copy.start)
            if bending and c in RELAYED:
                out, _, from_here, _ = legs(s, t, c)[way]
                under(from_here, out.start)

    def wait_in(s, *key):
        for copy, _, has_in in plans[s].get(key, ()):
            under(has_in, copy.wait_recv)

    def drain(s, t):
        for key, row in plans[s].items():
            if key[1] == t:
                for copy, has_out, _ in row:
                    under(has_out, copy.wait_send)
        if bending:
            for c in RELAYED:
                for out, on, from_here, here in legs(s, t, c):
                    under(from_here, out.wait_send)
                    under(here, on.wait_send)

    def v_parts(buf, t):
        eps = eps_of(d_speed)
        coef = ACCEL_MAX / (3.0 * d_speed)
        e4 = np.float32(np.float32(eps * eps) ** 2)
        lane = lax.broadcasted_iota(jnp.int32, (8, nv), 1)
        edge = lane == 0
        keep = jnp.where((lane == 0) | (lane == nv - 1), 0.0, 1.0)
        inner_lane = jnp.where(edge, 0.0, 1.0)
        rows, rows_acc = tile_rows(t), slice(8 * t, 8 * t + 8)

        def first(x, half):
            for j in range(group):
                u = buf[3 + x, 3 + half * group + j, rows, :]
                q = u - pltpu.roll(u, 1, 1)
                va[half, 0, j] = q
                va[half, 1, j] = ((pltpu.roll(u, nv - 1, 1) - u) - q) * keep

        def second(half):
            for j in range(group):
                q, d = va[half, 0, j], va[half, 1, j]
                vb[half, 0, j] = pltpu.roll(d, 2, 1)
                vb[half, 1, j] = pltpu.roll(d, 1, 1)
                vb[half, 2, j] = d
                vb[half, 3, j] = pltpu.roll(d, nv - 1, 1)
                vb[half, 4, j] = pltpu.roll(q, 1, 1)
                vb[half, 5, j] = q
                vb[half, 6, j] = pltpu.roll(q, nv - 1, 1)

        def third(x, half):
            for j in range(group):
                k = half * group + j
                d1, d2, d3, d4, qb, qc, qd = [vb[half, i, j] for i in range(7)]
                e1 = d2 - d1
                e2 = d3 - d2
                e3 = d4 - d3
                s1, s2, s3 = smooth(d2, d3, e1, e2, e3, eps)
                t1 = s2 * s3
                t2 = s1 * s3
                t3 = s1 * s2
                r1 = t1 * t1
                r2 = t2 * t2
                r3 = t3 * t3
                f12 = e1 - e2
                f23 = e2 - e3
                r2l = jnp.where(edge, r1, r2)
                r3l = jnp.where(edge, e4, r3)
                r2r = jnp.where(edge, r3, r2)
                r1r = jnp.where(edge, e4, r1)
                cl = jnp.where(edge, qd, qc)
                cr = jnp.where(edge, qb, qc)
                nl = r1 * (f12 * inner_lane) + 1.5 * (r3l * f23)
                nr = 1.5 * (r1r * f12) + r3 * (f23 * inner_lane)
                left = (3.0 * cl + (d3 + 0.5 * d2)) + nl * rcp(r1 + 6.0 * r2l + 3.0 * r3l)
                right = ((d2 + 0.5 * d3) - 3.0 * cr) + nr * rcp(3.0 * r1r + 6.0 * r2r + r3)
                acc[x, k, rows_acc, :] = coef * left
                rights[x, k, rows_acc, :] = coef * right

        def begin():
            first(0, 0)
            first(0, 1)
            second(0)

        def body(x, carry):
            after = jnp.minimum(x + 1, nx - 1)
            third(x, 0)
            second(1)
            first(after, 0)
            third(x, 1)
            second(0)
            first(after, 1)
            return carry

        return begin, body

    def v_pass(buf, t):
        begin, body = v_parts(buf, t)
        begin()
        lax.fori_loop(0, nx, body, 0)

    def h_pass(s, t):
        buf = bufs[s]
        eps = eps_of(d_theta)
        coef = TURN_MAX / (3.0 * d_theta)
        rows, rows_acc = tile_rows(t), pl.ds(8 * t, 8)

        def body(x, carry):
            dt = step[...]
            u = [buf[3 + x, j, rows, :] for j in range(nh + 6)]
            q = [u[j + 1] - u[j] for j in range(nh + 5)]
            d = [q[j + 1] - q[j] for j in range(nh + 4)]
            tr = [triple(d[j], d[j + 1], eps) for j in range(nh + 3)]
            before = None
            for f in range(nh + 1):
                left, right = face_pair(
                    q[f + 2], d[f + 1], d[f + 2], tr[f][0], tr[f + 1][0], tr[f + 2][0],
                    tr[f][1], tr[f + 1][2], tr[f + 2][3])
                if before is not None:
                    k = f - 1
                    total = acc[x, k, rows_acc, :] + coef * jnp.minimum(before, right)
                    moved = u[k + 3] - dt * jnp.maximum(total, 0.0)
                    if s == 0:
                        b1[3 + x, 3 + k, rows, :] = moved
                    elif s == 1:
                        b2[3 + x, 3 + k, rows, :] = 0.75 * b0[3 + x, 3 + k, rows, :] + 0.25 * moved
                    else:
                        out_ref[x, k, rows_acc, :] = (moved - b0[3 + x, 3 + k, rows, :]) * (2.0 / (3.0 * SCALE))
                before = left
            return carry

        for c, (x0, count) in enumerate(planes):
            wait_in(s, "h", t, c)
            lax.fori_loop(x0, x0 + count, body, 0)
            if s < 2:
                send(s + 1, "h", t, c)
                if c == 0:
                    send_x(s + 1, t, 1)
                if c == len(planes) - 1:
                    send_x(s + 1, t, 0)
                send(s + 1, "y", t, c)

    def flow_row(comp, k):
        return flow_ref[comp, pl.ds(ha * nh + k, 1), :]

    def y_parts(s, t):
        buf = bufs[s]
        eps = eps_of(CELL_SIZE)
        rows = slice(8 * t, 8 * t + 8)

        def begin():
            for c in range(len(planes)):
                if t == 0:
                    for copy, _, has_in in plans[s]["y", tiles - 1, c][:1]:
                        under(has_in, copy.wait_recv)
                if t == tiles - 1:
                    for copy, _, has_in in plans[s]["y", 0, c][-1:]:
                        under(has_in, copy.wait_recv)

        def body(x, carry):
            for k in range(nh):
                u = [buf[3 + x, 3 + k, PAD + 8 * t + j:PAD + 8 * t + j + 8, :] for j in range(-3, 4)]
                q = [u[j + 1] - u[j] for j in range(6)]
                d = [q[j + 1] - q[j] for j in range(5)]
                fh = flow_row(1, k) + wind[1, x, rows, :]
                along_v = jnp.minimum(acc[x, k, rows, :], pltpu.roll(rights[x, k, rows, :], nv - 1, 1))
                acc[x, k, rows, :] = along_v + upwind(*d, q[2], q[3], fh, eps)
            return carry

        return begin, body

    def y_pass(s, t):
        begin, body = y_parts(s, t)
        begin()
        lax.fori_loop(0, nx, body, 0)

    def yv_pass(s, t):
        y_begin, y_body = y_parts(s, t)
        v_begin, v_body = v_parts(bufs[s], t + 1)
        v_begin()
        y_begin()

        def body(x, carry):
            y_body(x, carry)
            v_body(x, carry)
            return carry

        lax.fori_loop(0, nx, body, 0)

    def x_pass(s, t):
        buf = bufs[s]
        eps = eps_of(CELL_SIZE)
        rows, rows_acc = tile_rows(t), pl.ds(8 * t, 8)

        def body(k, carry):
            row = flow_row(0, k)
            u = [buf[j, 3 + k, rows, :] for j in range(nx + 6)]
            q = [u[j + 1] - u[j] for j in range(nx + 5)]
            d = [q[j + 1] - q[j] for j in range(nx + 4)]
            for x in range(nx):
                fh = row + wind[0, x, rows_acc, :]
                acc[x, k, rows_acc, :] += upwind(*d[x:x + 5], q[x + 2], q[x + 3], fh, eps)
            return carry

        for c, (k0, count) in enumerate(heads):
            wait_in(s, "x", t, c)
            lax.fori_loop(k0, k0 + count, body, 0)

    def fill_x(buf, t):
        rows = tile_rows(t)

        def ends(low):
            def act():
                def body(k, carry):
                    edge = buf[3 if low else nx + 2, 3 + k, rows, :]
                    slope = edge - buf[4 if low else nx + 1, 3 + k, rows, :]
                    for r in range(1, 4):
                        buf[3 - r if low else nx + 2 + r, 3 + k, rows, :] = edge + r * slope
                    return carry
                lax.fori_loop(0, nh, body, 0)
            return act
        pl.when(gx == 0)(ends(True))
        pl.when(gx == ngx - 1)(ends(False))

    def fill_y(buf, t):
        index = lax.broadcasted_iota(jnp.int32, (8, nv), 0).astype(jnp.float32)

        def ends(low):
            reach = (8.0 - index) if low else (index + 1.0)
            at, near, to = (PAD, PAD + 1, 0) if low else (PAD + ny - 1, PAD + ny - 2, PAD + ny)

            def act():
                def body(x, carry):
                    for k in range(nh):
                        edge = buf[3 + x, 3 + k, at:at + 1, :]
                        slope = edge - buf[3 + x, 3 + k, near:near + 1, :]
                        buf[3 + x, 3 + k, to:to + 8, :] = edge + reach * slope
                    return carry
                lax.fori_loop(0, nx, body, 0)
            return act
        if t == 0:
            pl.when(gy == 0)(ends(True))
        if t == tiles - 1:
            pl.when(gy == ngy - 1)(ends(False))

    def open_x(t, far):
        for c in range(len(heads)):
            if far and c in RELAYED:
                continue
            for way, (copy, _, _) in enumerate(plans[0]["x", t, c]):
                under(gx == 1 + way if far else lax.rem(gx, 2) == way, copy.start)
            if c in RELAYED:
                for out, _, from_here, _ in legs(0, t, c):
                    under(from_here, out.start)

    def open_h(t, far):
        for p in range(len(planes)):
            for way, (copy, _, _) in enumerate(plans[0]["h", t, p]):
                edge = (nha - 1) * (1 - way)
                under(ha == edge if far else ha != edge, copy.start)

    def open_y(t):
        for c in range(len(planes)):
            send(0, "y", t, c)

    def open_tile(t, along_x=True, along_h=True):
        if bending and along_x:
            open_x(t, False)
            open_x(t, True)
        if bending and along_h:
            for p in range(1, len(planes)):
                for way, (copy, _, _) in enumerate(plans[0]["h", t, p]):
                    under(ha != (nha - 1) * (1 - way), copy.start)
            open_h(t, True)

    if bending:
        open_h(0, False)
        open_x(0, False)
        open_y(tiles - 1)
        signal(far_x, {"gx": beside})()
        under(ha == 1, signal(low_in, {"ha": ha + 1}))
        under(ha == nha - 2, signal(high_in, {"ha": ha - 1}))
        open_y(0) if tiles > 1 else None

        @pl.when((ha > 1) & (ha < nha - 1))
        def _():
            await_one(low_in)()
            signal(low_in, {"ha": ha + 1})()

        @pl.when((ha > 0) & (ha < nha - 2))
        def _():
            await_one(high_in)()
            signal(high_in, {"ha": ha - 1})()

        await_one(far_x)()
        open_x(0, True)
        for t in range(1, tiles):
            for way, (copy, _, _) in enumerate(plans[0]["h", t, 0]):
                under(ha != (nha - 1) * (1 - way), copy.start)
        for copy in rate_copies:
            copy.start()
        v_pass(b0, 0)
        under(ha == nha - 1, await_one(low_in))
        under(ha == 0, await_one(high_in))
        open_h(0, True)
    else:
        for t in range(tiles):
            for p in range(len(planes)):
                send(0, "h", t, p)
                send(0, "y", t, p)
            for way in range(2):
                send_x(0, t, way)
        for copy in rate_copies:
            copy.start()
        v_pass(b0, 0)
    for s in range(3):
        fill_y(bufs[s], 0)
        fill_y(bufs[s], tiles - 1) if tiles > 1 else None
        for t in range(1, tiles):
            yv_pass(s, t - 1)
            if s == 0:
                forward(s, t - 1)
                open_tile(t)
        y_pass(s, tiles - 1)
        if tiles == 1:
            forward(s, 0)
        for t in range(tiles):
            fill_x(bufs[s], t)
            x_pass(s, t)
            if t == 0 and tiles > 1:
                forward(s, tiles - 1)
            if s == 0 and t == 0:
                settle_rate()
            if s < 2 and t > 0:
                forward(s + 1, t - 1)
            h_pass(s, t)
            if s == 2 and t == max(tiles - 2, 0):
                for copy in rate_copies:
                    copy.wait_send()
                for done in range(3 * tiles - 1):
                    drain(done // tiles, done % tiles)
            if s < 2 and t == 0:
                v_pass(bufs[s + 1], 0)

    drain(2, tiles - 1)


def tables(nv, n_head):
    speeds = (SPEED_LOW + SPEED_SPAN * (np.arange(nv, dtype=np.float32) + np.float32(0.5)) / nv).astype(np.float32)
    angles = np.arange(n_head, dtype=np.float32) * np.float32(2.0 * math.pi / n_head)
    turns = np.stack([np.cos(angles.astype(np.float64)), np.sin(angles.astype(np.float64))])
    flow = (turns[:, :, None] * speeds[None, None, :] / CELL_SIZE).astype(np.float32)
    ends = np.concatenate([flow[:, :, 0], flow[:, :, -1]], axis=1)
    rows = -(-ends.shape[1] // 128)
    ends = np.concatenate([ends, np.repeat(ends[:, :1], rows * 128 - ends.shape[1], axis=1)], axis=1)
    return flow, ends.reshape(2, rows, 128)


def solution(mesh):
    axes = (mesh.shape["gx"], mesh.shape["gy"], mesh.shape["ha"])

    def body(level_set, wind_field):
        nx, ny, nh, nv = level_set.shape
        flow, ends = tables(nv, nh * axes[2])
        n_xy = axes[0] * axes[1]
        tiles = ny // 8
        count = n_copies(nx, nh, tiles)
        state = pltpu.VMEM((nx + 6, nh + 6, ny + 2 * PAD, nv), jnp.float32)
        cells = pltpu.VMEM((nx, nh, ny, nv), jnp.float32)
        vmem = pl.BlockSpec(memory_space=pltpu.VMEM)
        increment = pl.pallas_call(
            functools.partial(kernel, (nx, ny, nh, nv), axes),
            out_shape=pltpu.VMEM((nx, nh, ny, nv), jnp.float32),
            in_specs=[pl.BlockSpec(memory_space=pltpu.HBM)] * 4,
            out_specs=vmem,
            scratch_shapes=[
                state, state, state, cells, cells, cells,
                pltpu.SMEM((2, nx, ny), jnp.float32),
                pltpu.VMEM(flow.shape, jnp.float32),
                pltpu.VMEM(ends.shape, jnp.float32),
                pltpu.VMEM((2, 2, nh // 2, 8, nv), jnp.float32),
                pltpu.VMEM((2, 7, nh // 2, 8, nv), jnp.float32),
                pltpu.VMEM((2, nx, ny, nv), jnp.float32),
                pltpu.VMEM((8, 128), jnp.float32),
                pltpu.VMEM((n_xy - 1, 8, 128), jnp.float32),
                pltpu.VMEM((8, nv), jnp.float32),
                pltpu.VMEM((3, 3, nh, ny, nv), jnp.float32),
                pltpu.SemaphoreType.DMA((3, count)),
                pltpu.SemaphoreType.DMA((3, count)),
                pltpu.SemaphoreType.DMA((n_xy - 1,)),
                pltpu.SemaphoreType.DMA((n_xy - 1,)),
                pltpu.SemaphoreType.DMA((4,)),
                pltpu.SemaphoreType.DMA((3, tiles, len(RELAYED), 2)),
                pltpu.SemaphoreType.DMA((3, tiles, len(RELAYED), 2)),
                pltpu.SemaphoreType.REGULAR,
                pltpu.SemaphoreType.REGULAR,
                pltpu.SemaphoreType.REGULAR,
            ],
            compiler_params=pltpu.CompilerParams(
                collective_id=0, has_side_effects=True, vmem_limit_bytes=56 * 2**20
            ),
        )(level_set.transpose(0, 2, 1, 3), wind_field, jnp.asarray(flow), jnp.asarray(ends))
        return increment.transpose(0, 2, 1, 3)

    return jax.shard_map(
        body,
        mesh=mesh,
        in_specs=(P("gx", "gy", "ha", None), P(None, "gx", "gy")),
        out_specs=P("gx", "gy", "ha", None),
        check_vma=False,
    )
```

```python
import functools
import math

import jax
import jax.numpy as jnp
import numpy as np
from jax import lax
from jax.experimental import pallas as pl
from jax.experimental.pallas import tpu as pltpu
from jax.sharding import PartitionSpec as P

CELL_SIZE = 0.05
SPEED_LOW = 0.1
SPEED_SPAN = 0.4
TURN_MAX = 1.0
ACCEL_MAX = 0.05
CFL_NUMBER = 0.5
WENO_EPS = 1e-06
SCALE = 32.0
PAD = 8
MESH = pl.DeviceIdType.MESH


def rcp(d):
    return pl.reciprocal(d, approx=False)


def eps_of(spacing):
    return 0.75 * WENO_EPS * (spacing * SCALE) ** 2


def smooth(d2, d3, e1, e2, e3, eps):
    g2 = 0.75 * d2
    g3 = 0.75 * d3
    c3 = g3 * d3 + eps
    s1 = e1 * (e1 + g2) + (g2 * d2 + eps)
    s2 = e2 * (e2 - g3) + c3
    s3 = e3 * (e3 - g3) + c3
    return s1, s2, s3


def upwind(dm2, dm1, d0, dp1, dp2, c0, c1, fh, eps):
    pos = fh > 0.0
    d1 = jnp.where(pos, dp2, dm2)
    d2 = jnp.where(pos, dp1, dm1)
    d4 = jnp.where(pos, dm1, dp1)
    c = jnp.where(pos, c1, c0)
    d3 = d0
    e1 = d2 - d1
    e2 = d3 - d2
    e3 = d4 - d3
    s1, s2, s3 = smooth(d2, d3, e1, e2, e3, eps)
    t1 = s2 * s3
    t2 = s1 * s3
    t3 = s1 * s2
    r1 = t1 * t1
    r2 = t2 * t2
    w3 = 1.5 * (t3 * t3)
    num = r1 * (e1 - e2) + w3 * (e2 - e3)
    den = (r1 + 6.0 * r2) + (w3 + w3)
    q = (d3 + 0.5 * d2) + num * rcp(den)
    return q * (jnp.abs(fh) * (1.0 / 3.0)) - c * fh


def triple(da, db, eps):
    e = db - da
    s2 = e * e + (0.75 * (da * db) + eps)
    h = 1.5 * e
    return e, s2 + db * h, s2, s2 - da * h


def face_pair(c, d2, d3, e1, e2, e3, s1, s2, s3):
    t1 = s2 * s3
    t2 = s1 * s3
    t3 = s1 * s2
    r1 = t1 * t1
    r2 = t2 * t2
    r3 = t3 * t3
    a = r1 * (e1 - e2)
    b = r3 * (e2 - e3)
    m = 6.0 * r2 + (r1 + r3)
    n = a + b
    left = (3.0 * c + (d3 + 0.5 * d2)) + (n + 0.5 * b) * rcp(m + (r3 + r3))
    right = ((d2 + 0.5 * d3) - 3.0 * c) + (n + 0.5 * a) * rcp(m + (r1 + r1))
    return left, right


def head_chunks(nh):
    half = nh - nh * 2 // 5
    return ((0, half), (half, nh - half))


RELAYED = (1,)


def folded(axes):
    return axes[0] == 4 and axes[1] == 2 and axes[2] > 2


def plane_chunks(nx):
    half = nx // 2
    return ((0, half), (half, nx - half))


def n_copies(nx, nh, tiles):
    return 2 * len(plane_chunks(nx)) * (tiles + 1) + 2 * len(head_chunks(nh)) * tiles


def kernel(sizes, axes, u_hbm, wind_hbm, flow_hbm, rate_hbm, out_ref,
           b0, b1, b2, acc, rights, u_ref, wind_ref, flow_ref, rate_ref, va, vb, wind, best, peers, step, relay,
           sends, recvs, rsend, rrecv, isem, lsend, lrecv, far_x, low_in, high_in):
    nx, ny, nh, nv = sizes
    ngx, ngy, nha = axes
    bufs = (b0, b1, b2)
    d_theta = 2.0 * math.pi / (nh * nha)
    d_speed = SPEED_SPAN / nv
    tiles = ny // 8
    group = nh // 2
    heads, planes = head_chunks(nh), plane_chunks(nx)
    gx, gy, ha = lax.axis_index("gx"), lax.axis_index("gy"), lax.axis_index("ha")
    n_xy = ngx * ngy
    me = gx * ngy + gy

    def peer(delta):
        other = lax.rem(me + delta, n_xy)
        return {"gx": other // ngy, "gy": lax.rem(other, ngy)}

    up_ha = {"ha": lax.rem(ha + 1, nha)}
    down_ha = {"ha": lax.rem(ha + nha - 1, nha)}
    bending = folded(axes)
    beside, across = gx + 1 - 2 * lax.rem(gx, 2), lax.rem(gx + 2, 4)
    near = ({"gy": 1 - gy}, {"gx": beside}, {"gx": across},
            {"gx": beside, "gy": 1 - gy}, {"gx": across, "gy": 1 - gy})

    def under(condition, act):
        if condition is None:
            act()
        else:
            pl.when(condition)(act)

    def signal(semaphore, target):
        return lambda: pl.semaphore_signal(semaphore, inc=1, device_id=target, device_id_type=MESH)

    def await_one(semaphore):
        return lambda: pl.semaphore_wait(semaphore, 1)

    barrier = pltpu.get_barrier_semaphore()
    if bending:
        for target in near:
            signal(barrier, target)()
        under(ha < nha - 1, signal(barrier, {"ha": ha + 1}))
        under(ha > 0, signal(barrier, {"ha": ha - 1}))
    else:
        for delta in range(1, n_xy):
            signal(barrier, peer(delta))()
        for target in (up_ha, down_ha):
            signal(barrier, target)()

    fetches = [
        pltpu.make_async_copy(src, dst, isem.at[i])
        for i, (src, dst) in enumerate((
            (wind_hbm, wind_ref), (rate_hbm, rate_ref), (u_hbm, u_ref), (flow_hbm, flow_ref)))
    ]
    for fetch in fetches:
        fetch.start()
    for fetch in fetches:
        fetch.wait()

    def load_plane(x, carry):
        for k in range(nh):
            b0[3 + x, 3 + k, PAD:PAD + ny, :] = u_ref[x, k] * SCALE
        for comp in range(2):
            for y in range(ny):
                wind[comp, x, y:y + 1, :] = jnp.full((1, nv), wind_ref[comp, x, y] * (1.0 / CELL_SIZE), jnp.float32)
        return carry

    lax.fori_loop(0, nx, load_plane, 0)

    def rate_plane(x, top):
        for r in range(rate_ref.shape[1]):
            for t in range(tiles):
                fx = rate_ref[0, r:r + 1, :] + wind[0, x, 8 * t:8 * t + 8, :]
                fy = rate_ref[1, r:r + 1, :] + wind[1, x, 8 * t:8 * t + 8, :]
                top = jnp.maximum(top, jnp.abs(fx) + jnp.abs(fy))
        return top

    best[...] = lax.fori_loop(0, nx, rate_plane, jnp.zeros((8, 128), jnp.float32))

    if bending:
        beyond = (ha + nha - 2) // (nha - 1) + (2 * nha - 3 - ha) // (nha - 1)
        pl.semaphore_wait(barrier, len(near) + beyond)
    else:
        pl.semaphore_wait(barrier, n_xy + 1)

    def tile_rows(t):
        return pl.ds(PAD + 8 * t, 8)

    places = []

    def copies(s):
        buf = bufs[s]
        plans = {}
        for t in range(tiles):
            ys = tile_rows(t)
            for c, (x0, count) in enumerate(planes):
                xs = pl.ds(3 + x0, count)
                plans["h", t, c] = (
                    (buf.at[xs, pl.ds(nh, 3), ys], buf.at[xs, pl.ds(0, 3), ys], up_ha, None, None),
                    (buf.at[xs, pl.ds(3, 3), ys], buf.at[xs, pl.ds(3 + nh, 3), ys], down_ha, None, None),
                )
            for c, (k0, count) in enumerate(heads):
                hc = pl.ds(3 + k0, count)
                around = bending and c in RELAYED
                plans["x", t, c] = (
                    (buf.at[pl.ds(nx, 3), hc, ys], buf.at[pl.ds(0, 3), hc, ys], {"gx": gx + 1},
                     (gx == 0) | (gx == 2) if around else gx < ngx - 1, gx > 0),
                    (buf.at[pl.ds(3, 3), hc, ys], buf.at[pl.ds(3 + nx, 3), hc, ys], {"gx": gx - 1},
                     (gx == 1) | (gx == 3) if around else gx > 0, gx < ngx - 1),
                )
        hc = pl.ds(3, nh)
        for c, (x0, count) in enumerate(planes):
            xs = pl.ds(3 + x0, count)
            plans["y", tiles - 1, c] = (
                (buf.at[xs, hc, pl.ds(ny, PAD)], buf.at[xs, hc, pl.ds(0, PAD)], {"gy": gy + 1},
                 gy < ngy - 1, gy > 0),
            )
            plans["y", 0, c] = plans.get(("y", 0, c), ()) + (
                (buf.at[xs, hc, pl.ds(PAD, PAD)], buf.at[xs, hc, pl.ds(PAD + ny, PAD)], {"gy": gy - 1},
                 gy > 0, gy < ngy - 1),
            )
        made, at, starts = {}, 0, {}
        for key, group_of in plans.items():
            row = []
            starts[key] = at
            for src, dst, target, has_out, has_in in group_of:
                row.append((pltpu.make_async_remote_copy(
                    src_ref=src, dst_ref=dst, send_sem=sends.at[s, at], recv_sem=recvs.at[s, at],
                    device_id=target, device_id_type=MESH), has_out, has_in))
                at += 1
            made[key] = row
        places.append(starts)
        return made

    rate_copies = [
        pltpu.make_async_remote_copy(
            src_ref=best, dst_ref=peers.at[delta - 1], send_sem=rsend.at[delta - 1],
            recv_sem=rrecv.at[delta - 1], device_id=peer(delta), device_id_type=MESH)
        for delta in range(1, n_xy)
    ]

    def settle_rate():
        top = best[...]
        for i, copy in enumerate(rate_copies):
            copy.wait_recv()
            top = jnp.maximum(top, peers[i])
        rate = jnp.max(top, axis=(0, 1), keepdims=True) + (TURN_MAX / d_theta + ACCEL_MAX / d_speed)
        step[...] = jnp.broadcast_to(CFL_NUMBER / rate, step.shape)

    plans = [copies(s) for s in range(3)]

    built = {}

    def legs(s, t, c):
        if (s, t, c) in built:
            return built[s, t, c]
        buf = bufs[s]
        k0, count = heads[c]
        hc, ys = pl.ds(3 + k0, count), tile_rows(t)
        held = relay.at[s, pl.ds(0, 3), pl.ds(k0, count), pl.ds(8 * t, 8)]
        i = RELAYED.index(c)
        rows = []
        for way, (src, dst, origin, middle, end) in enumerate((
            (buf.at[pl.ds(nx, 3), hc, ys], buf.at[pl.ds(0, 3), hc, ys], 1, 3, 2),
            (buf.at[pl.ds(3, 3), hc, ys], buf.at[pl.ds(3 + nx, 3), hc, ys], 2, 0, 1),
        )):
            out = pltpu.make_async_remote_copy(
                src_ref=src, dst_ref=held, send_sem=lsend.at[s, t, i, way], recv_sem=lrecv.at[s, t, i, way],
                device_id={"gx": middle}, device_id_type=MESH)
            on = pltpu.make_async_remote_copy(
                src_ref=held, dst_ref=dst, send_sem=sends.at[s, places[s]["x", t, c] + way],
                recv_sem=recvs.at[s, places[s]["x", t, c] + way],
                device_id={"gx": end}, device_id_type=MESH)
            rows.append((out, on, gx == origin, gx == middle))
        built[s, t, c] = rows
        return rows

    def forward(s, t):
        if bending:
            for c in RELAYED:
                for out, on, _, here in legs(s, t, c):
                    @pl.when(here)
                    def _():
                        out.wait_recv()
                        on.start()

    def send(s, *key):
        for copy, has_out, _ in plans[s].get(key, ()):
            under(has_out, copy.start)

    def send_x(s, t, way):
        for c in range(len(heads)):
            copy, has_out, _ = plans[s]["x", t, c][way]
            under(has_out, copy.start)
            if bending and c in RELAYED:
                out, _, from_here, _ = legs(s, t, c)[way]
                under(from_here, out.start)

    def wait_in(s, *key):
        for copy, _, has_in in plans[s].get(key, ()):
            under(has_in, copy.wait_recv)

    def drain(s, t):
        for key, row in plans[s].items():
            if key[1] == t:
                for copy, has_out, _ in row:
                    under(has_out, copy.wait_send)
        if bending:
            for c in RELAYED:
                for out, on, from_here, here in legs(s, t, c):
                    under(from_here, out.wait_send)
                    under(here, on.wait_send)

    def v_parts(buf, t):
        eps = eps_of(d_speed)
        coef = ACCEL_MAX / (3.0 * d_speed)
        e4 = np.float32(np.float32(eps * eps) ** 2)
        lane = lax.broadcasted_iota(jnp.int32, (8, nv), 1)
        edge = lane == 0
        keep = jnp.where((lane == 0) | (lane == nv - 1), 0.0, 1.0)
        inner_lane = jnp.where(edge, 0.0, 1.0)
        rows, rows_acc = tile_rows(t), slice(8 * t, 8 * t + 8)

        def first(x, half):
            for j in range(group):
                u = buf[3 + x, 3 + half * group + j, rows, :]
                q = u - pltpu.roll(u, 1, 1)
                va[half, 0, j] = q
                va[half, 1, j] = ((pltpu.roll(u, nv - 1, 1) - u) - q) * keep

        def second(half):
            for j in range(group):
                q, d = va[half, 0, j], va[half, 1, j]
                vb[half, 0, j] = pltpu.roll(d, 2, 1)
                vb[half, 1, j] = pltpu.roll(d, 1, 1)
                vb[half, 2, j] = d
                vb[half, 3, j] = pltpu.roll(d, nv - 1, 1)
                vb[half, 4, j] = pltpu.roll(q, 1, 1)
                vb[half, 5, j] = q
                vb[half, 6, j] = pltpu.roll(q, nv - 1, 1)

        def third(x, half):
            for j in range(group):
                k = half * group + j
                d1, d2, d3, d4, qb, qc, qd = [vb[half, i, j] for i in range(7)]
                e1 = d2 - d1
                e2 = d3 - d2
                e3 = d4 - d3
                s1, s2, s3 = smooth(d2, d3, e1, e2, e3, eps)
                t1 = s2 * s3
                t2 = s1 * s3
                t3 = s1 * s2
                r1 = t1 * t1
                r2 = t2 * t2
                r3 = t3 * t3
                f12 = e1 - e2
                f23 = e2 - e3
                r2l = jnp.where(edge, r1, r2)
                r3l = jnp.where(edge, e4, r3)
                r2r = jnp.where(edge, r3, r2)
                r1r = jnp.where(edge, e4, r1)
                cl = jnp.where(edge, qd, qc)
                cr = jnp.where(edge, qb, qc)
                nl = r1 * (f12 * inner_lane) + 1.5 * (r3l * f23)
                nr = 1.5 * (r1r * f12) + r3 * (f23 * inner_lane)
                left = (3.0 * cl + (d3 + 0.5 * d2)) + nl * rcp(r1 + 6.0 * r2l + 3.0 * r3l)
                right = ((d2 + 0.5 * d3) - 3.0 * cr) + nr * rcp(3.0 * r1r + 6.0 * r2r + r3)
                acc[x, k, rows_acc, :] = coef * left
                rights[x, k, rows_acc, :] = coef * right

        def begin():
            first(0, 0)
            first(0, 1)
            second(0)

        def body(x, carry):
            after = jnp.minimum(x + 1, nx - 1)
            third(x, 0)
            second(1)
            first(after, 0)
            third(x, 1)
            second(0)
            first(after, 1)
            return carry

        return begin, body

    def v_pass(buf, t):
        begin, body = v_parts(buf, t)
        begin()
        lax.fori_loop(0, nx, body, 0)

    def h_pass(s, t):
        buf = bufs[s]
        eps = eps_of(d_theta)
        coef = TURN_MAX / (3.0 * d_theta)
        rows, rows_acc = tile_rows(t), pl.ds(8 * t, 8)

        def body(x, carry):
            dt = step[...]
            u = [buf[3 + x, j, rows, :] for j in range(nh + 6)]
            q = [u[j + 1] - u[j] for j in range(nh + 5)]
            d = [q[j + 1] - q[j] for j in range(nh + 4)]
            tr = [triple(d[j], d[j + 1], eps) for j in range(nh + 3)]
            before = None
            for f in range(nh + 1):
                left, right = face_pair(
                    q[f + 2], d[f + 1], d[f + 2], tr[f][0], tr[f + 1][0], tr[f + 2][0],
                    tr[f][1], tr[f + 1][2], tr[f + 2][3])
                if before is not None:
                    k = f - 1
                    total = acc[x, k, rows_acc, :] + coef * jnp.minimum(before, right)
                    moved = u[k + 3] - dt * jnp.maximum(total, 0.0)
                    if s == 0:
                        b1[3 + x, 3 + k, rows, :] = moved
                    elif s == 1:
                        b2[3 + x, 3 + k, rows, :] = 0.75 * b0[3 + x, 3 + k, rows, :] + 0.25 * moved
                    else:
                        out_ref[x, k, rows_acc, :] = (moved - b0[3 + x, 3 + k, rows, :]) * (2.0 / (3.0 * SCALE))
                before = left
            return carry

        for c, (x0, count) in enumerate(planes):
            wait_in(s, "h", t, c)
            lax.fori_loop(x0, x0 + count, body, 0)
            if s < 2:
                send(s + 1, "h", t, c)
                if c == 0:
                    send_x(s + 1, t, 1)
                if c == len(planes) - 1:
                    send_x(s + 1, t, 0)
                send(s + 1, "y", t, c)

    def flow_row(comp, k):
        return flow_ref[comp, pl.ds(ha * nh + k, 1), :]

    def y_parts(s, t):
        buf = bufs[s]
        eps = eps_of(CELL_SIZE)
        rows = slice(8 * t, 8 * t + 8)

        def begin():
            for c in range(len(planes)):
                if t == 0:
                    for copy, _, has_in in plans[s]["y", tiles - 1, c][:1]:
                        under(has_in, copy.wait_recv)
                if t == tiles - 1:
                    for copy, _, has_in in plans[s]["y", 0, c][-1:]:
                        under(has_in, copy.wait_recv)

        def body(x, carry):
            for k in range(nh):
                u = [buf[3 + x, 3 + k, PAD + 8 * t + j:PAD + 8 * t + j + 8, :] for j in range(-3, 4)]
                q = [u[j + 1] - u[j] for j in range(6)]
                d = [q[j + 1] - q[j] for j in range(5)]
                fh = flow_row(1, k) + wind[1, x, rows, :]
                along_v = jnp.minimum(acc[x, k, rows, :], pltpu.roll(rights[x, k, rows, :], nv - 1, 1))
                acc[x, k, rows, :] = along_v + upwind(*d, q[2], q[3], fh, eps)
            return carry

        return begin, body

    def y_pass(s, t):
        begin, body = y_parts(s, t)
        begin()
        lax.fori_loop(0, nx, body, 0)

    def yv_pass(s, t):
        y_begin, y_body = y_parts(s, t)
        v_begin, v_body = v_parts(bufs[s], t + 1)
        v_begin()
        y_begin()

        def body(x, carry):
            y_body(x, carry)
            v_body(x, carry)
            return carry

        lax.fori_loop(0, nx, body, 0)

    def x_pass(s, t):
        buf = bufs[s]
        eps = eps_of(CELL_SIZE)
        rows, rows_acc = tile_rows(t), pl.ds(8 * t, 8)

        def body(k, carry):
            row = flow_row(0, k)
            u = [buf[j, 3 + k, rows, :] for j in range(nx + 6)]
            q = [u[j + 1] - u[j] for j in range(nx + 5)]
            d = [q[j + 1] - q[j] for j in range(nx + 4)]
            for x in range(nx):
                fh = row + wind[0, x, rows_acc, :]
                acc[x, k, rows_acc, :] += upwind(*d[x:x + 5], q[x + 2], q[x + 3], fh, eps)
            return carry

        for c, (k0, count) in enumerate(heads):
            wait_in(s, "x", t, c)
            lax.fori_loop(k0, k0 + count, body, 0)

    def fill_x(buf, t):
        rows = tile_rows(t)

        def ends(low):
            def act():
                def body(k, carry):
                    edge = buf[3 if low else nx + 2, 3 + k, rows, :]
                    slope = edge - buf[4 if low else nx + 1, 3 + k, rows, :]
                    for r in range(1, 4):
                        buf[3 - r if low else nx + 2 + r, 3 + k, rows, :] = edge + r * slope
                    return carry
                lax.fori_loop(0, nh, body, 0)
            return act
        pl.when(gx == 0)(ends(True))
        pl.when(gx == ngx - 1)(ends(False))

    def fill_y(buf, t):
        index = lax.broadcasted_iota(jnp.int32, (8, nv), 0).astype(jnp.float32)

        def ends(low):
            reach = (8.0 - index) if low else (index + 1.0)
            at, near, to = (PAD, PAD + 1, 0) if low else (PAD + ny - 1, PAD + ny - 2, PAD + ny)

            def act():
                def body(x, carry):
                    for k in range(nh):
                        edge = buf[3 + x, 3 + k, at:at + 1, :]
                        slope = edge - buf[3 + x, 3 + k, near:near + 1, :]
                        buf[3 + x, 3 + k, to:to + 8, :] = edge + reach * slope
                    return carry
                lax.fori_loop(0, nx, body, 0)
            return act
        if t == 0:
            pl.when(gy == 0)(ends(True))
        if t == tiles - 1:
            pl.when(gy == ngy - 1)(ends(False))

    def open_x(t, far):
        for c in range(len(heads)):
            if far and c in RELAYED:
                continue
            for way, (copy, _, _) in enumerate(plans[0]["x", t, c]):
                under(gx == 1 + way if far else lax.rem(gx, 2) == way, copy.start)
            if c in RELAYED:
                for out, _, from_here, _ in legs(0, t, c):
                    under(from_here, out.start)

    def open_h(t, far):
        for p in range(len(planes)):
            for way, (copy, _, _) in enumerate(plans[0]["h", t, p]):
                edge = (nha - 1) * (1 - way)
                under(ha == edge if far else ha != edge, copy.start)

    def open_y(t):
        for c in range(len(planes)):
            send(0, "y", t, c)

    def open_tile(t, along_x=True, along_h=True):
        if bending and along_x:
            open_x(t, False)
            open_x(t, True)
        if bending and along_h:
            for p in range(1, len(planes)):
                for way, (copy, _, _) in enumerate(plans[0]["h", t, p]):
                    under(ha != (nha - 1) * (1 - way), copy.start)
            open_h(t, True)

    if bending:
        open_h(0, False)
        open_x(0, False)
        open_y(tiles - 1)
        signal(far_x, {"gx": beside})()
        under(ha == 1, signal(low_in, {"ha": ha + 1}))
        under(ha == nha - 2, signal(high_in, {"ha": ha - 1}))
        open_y(0) if tiles > 1 else None

        @pl.when((ha > 1) & (ha < nha - 1))
        def _():
            await_one(low_in)()
            signal(low_in, {"ha": ha + 1})()

        @pl.when((ha > 0) & (ha < nha - 2))
        def _():
            await_one(high_in)()
            signal(high_in, {"ha": ha - 1})()

        await_one(far_x)()
        open_x(0, True)
        for t in range(1, tiles):
            for way, (copy, _, _) in enumerate(plans[0]["h", t, 0]):
                under(ha != (nha - 1) * (1 - way), copy.start)
        for copy in rate_copies:
            copy.start()
        v_pass(b0, 0)
        under(ha == nha - 1, await_one(low_in))
        under(ha == 0, await_one(high_in))
        open_h(0, True)
    else:
        for t in range(tiles):
            for p in range(len(planes)):
                send(0, "h", t, p)
                send(0, "y", t, p)
            for way in range(2):
                send_x(0, t, way)
        for copy in rate_copies:
            copy.start()
        v_pass(b0, 0)
    for s in range(3):
        fill_y(bufs[s], 0)
        fill_y(bufs[s], tiles - 1) if tiles > 1 else None
        for t in range(1, tiles):
            yv_pass(s, t - 1)
            if s == 0:
                forward(s, t - 1)
                open_tile(t)
        y_pass(s, tiles - 1)
        if tiles == 1:
            forward(s, 0)
        for t in range(tiles):
            fill_x(bufs[s], t)
            x_pass(s, t)
            if t == 0 and tiles > 1:
                forward(s, tiles - 1)
            if s == 0 and t == 0:
                settle_rate()
            if s < 2 and t > 0:
                forward(s + 1, t - 1)
            h_pass(s, t)
            if s == 2 and t == max(tiles - 2, 0):
                for copy in rate_copies:
                    copy.wait_send()
                for done in range(3 * tiles - 1):
                    drain(done // tiles, done % tiles)
            if s < 2 and t == 0:
                v_pass(bufs[s + 1], 0)

    drain(2, tiles - 1)


def tables(nv, n_head):
    speeds = (SPEED_LOW + SPEED_SPAN * (np.arange(nv, dtype=np.float32) + np.float32(0.5)) / nv).astype(np.float32)
    angles = np.arange(n_head, dtype=np.float32) * np.float32(2.0 * math.pi / n_head)
    turns = np.stack([np.cos(angles.astype(np.float64)), np.sin(angles.astype(np.float64))])
    flow = (turns[:, :, None] * speeds[None, None, :] / CELL_SIZE).astype(np.float32)
    ends = np.concatenate([flow[:, :, 0], flow[:, :, -1]], axis=1)
    rows = -(-ends.shape[1] // 128)
    ends = np.concatenate([ends, np.repeat(ends[:, :1], rows * 128 - ends.shape[1], axis=1)], axis=1)
    return flow, ends.reshape(2, rows, 128)


def solution(mesh):
    axes = (mesh.shape["gx"], mesh.shape["gy"], mesh.shape["ha"])

    def body(level_set, wind_field):
        nx, ny, nh, nv = level_set.shape
        flow, ends = tables(nv, nh * axes[2])
        n_xy = axes[0] * axes[1]
        tiles = ny // 8
        count = n_copies(nx, nh, tiles)
        state = pltpu.VMEM((nx + 6, nh + 6, ny + 2 * PAD, nv), jnp.float32)
        cells = pltpu.VMEM((nx, nh, ny, nv), jnp.float32)
        vmem = pl.BlockSpec(memory_space=pltpu.VMEM)
        increment = pl.pallas_call(
            functools.partial(kernel, (nx, ny, nh, nv), axes),
            out_shape=pltpu.VMEM((nx, nh, ny, nv), jnp.float32),
            in_specs=[pl.BlockSpec(memory_space=pltpu.HBM)] * 4,
            out_specs=vmem,
            scratch_shapes=[
                state, state, state, cells, cells, cells,
                pltpu.SMEM((2, nx, ny), jnp.float32),
                pltpu.VMEM(flow.shape, jnp.float32),
                pltpu.VMEM(ends.shape, jnp.float32),
                pltpu.VMEM((2, 2, nh // 2, 8, nv), jnp.float32),
                pltpu.VMEM((2, 7, nh // 2, 8, nv), jnp.float32),
                pltpu.VMEM((2, nx, ny, nv), jnp.float32),
                pltpu.VMEM((8, 128), jnp.float32),
                pltpu.VMEM((n_xy - 1, 8, 128), jnp.float32),
                pltpu.VMEM((8, nv), jnp.float32),
                pltpu.VMEM((3, 3, nh, ny, nv), jnp.float32),
                pltpu.SemaphoreType.DMA((3, count)),
                pltpu.SemaphoreType.DMA((3, count)),
                pltpu.SemaphoreType.DMA((n_xy - 1,)),
                pltpu.SemaphoreType.DMA((n_xy - 1,)),
                pltpu.SemaphoreType.DMA((4,)),
                pltpu.SemaphoreType.DMA((3, tiles, len(RELAYED), 2)),
                pltpu.SemaphoreType.DMA((3, tiles, len(RELAYED), 2)),
                pltpu.SemaphoreType.REGULAR,
                pltpu.SemaphoreType.REGULAR,
                pltpu.SemaphoreType.REGULAR,
            ],
            compiler_params=pltpu.CompilerParams(
                collective_id=0, has_side_effects=True, vmem_limit_bytes=56 * 2**20
            ),
        )(level_set.transpose(0, 2, 1, 3), wind_field, jnp.asarray(flow), jnp.asarray(ends))
        return increment.transpose(0, 2, 1, 3)

    return jax.shard_map(
        body,
        mesh=mesh,
        in_specs=(P("gx", "gy", "ha", None), P(None, "gx", "gy")),
        out_specs=P("gx", "gy", "ha", None),
        check_vma=False,
    )
```
